32 devices in a mesh: mem: 8 (over z, x), geo: 4 (over y, core).
Axes of the slice: x: 2, y: 2, z: 4, core: 2. Of those that a mesh axis runs over, the one named last changes fastest.
Arguments:
- control: float32 [8, 32, 48, 384], P('mem', 'geo'), may hold values from -6 to 6
- kappa_table: float32 [16], replicated, may hold values from 0.02 to 0.24
- kappa_index: int32 [48, 384], replicated, may hold values from 0 to 15
- tile_bounds: int32 [5], replicated, may hold values from 0 to 18432, as said below
- filter_bands: float32 [4, 5, 32], replicated, may hold values from -0.3 to 0.3
- perturbation: bfloat16 [2, 8, 32, 18432], P(None, 'mem', None, 'geo'), may hold values from -6 to 6
Outputs:
- increment: float32 [2, 32, 18432], P(None, 'mem', 'geo')
The draws below stay inside these ranges and needn't reach their ends.
Inputs may be any that keep to these rules, and one draw needn't show every extreme that they name: tile_bounds[0] is 0, tile_bounds[4] is 18432, and the bounds never fall; tile t holds columns tile_bounds[t] to tile_bounds[t + 1] - 1.
All inputs are finite; a program needn't handle non-finite values.
Results may differ from the reference program's by a relative error of at most 0.005.
Values may be sent and summed in bfloat16 or wider, within the bound.
A program may use at most 64 MiB of HBM per device.

```python
import math
import jax
import jax.numpy as jnp
from jax import lax

LEV = 32
HX = 48
HY = 384
ITERS = 10
KAPPAS = 16
MEMBERS = 8
TILES = 4
NCOL = 18432


def draw_tile_bounds(key, part):
    widths = jax.random.randint(jax.random.fold_in(key, 7), (TILES,), 1, 5)
    cumulative = jnp.cumsum(widths).astype(jnp.int32)
    interior = HX * HY * cumulative // cumulative[-1]
    return jnp.concatenate([jnp.zeros((1,), jnp.int32), interior.astype(jnp.int32)])


def plant(array, key, least, largest):
    longest = array.shape.index(max(array.shape))
    spots = []
    for shift in (0, 1):
        where = [jax.random.randint(jax.random.fold_in(key, axis), (), 0, length) for axis, length in enumerate(array.shape)]
        where[longest] = (where[longest] + shift) % array.shape[longest]
        spots.append(tuple(where))
    return array.at[spots[0]].set(least).at[spots[1]].set(largest)


def raised(array, rng, source, target, parts, factor):
    owner, partner = [(jnp.arange(array.shape[position]) // (array.shape[position] // parts)).reshape([-1 if axis == position else 1 for axis in range(array.ndim)]) for position in (source, target)]
    chosen = jax.random.permutation(rng, parts)[partner]
    strong = (owner == chosen) | (owner == (partner + parts // 2) % parts)
    return jnp.where(strong, factor * array, array)


def shard_levels(own_key, dims, shards, least, high):
    gain = 1.0
    for axis_at, blocks in shards:
        steps = jax.random.uniform(jax.random.fold_in(jax.random.fold_in(own_key, 6), axis_at), (blocks,), jnp.float32, least / len(shards), high / len(shards))
        gain = gain * jnp.repeat(jnp.exp(steps), dims[axis_at] // blocks).reshape((-1,) + (1,) * (len(dims) - 1 - axis_at))
    return gain


def normal_values(stream_key, dims, spread, reach, cuts=(), kind=jnp.bfloat16):
    level = shard_levels(stream_key, dims, cuts, -0.22, 0.18) if cuts else 1.0
    entries = jax.random.normal(stream_key, dims, jnp.float32) * spread * level
    return jnp.minimum(jnp.maximum(entries, -reach), reach).astype(kind)


def heavy_noise(stream_key, extent, width, limit, pieces, heavy, kind=jnp.bfloat16):
    values = width * jax.random.normal(stream_key, extent, jnp.float32)
    if pieces:
        values = values * shard_levels(stream_key, extent, pieces, -0.22, 0.18)
    return jnp.clip(raised(values, jax.random.fold_in(stream_key, 3), *heavy), -limit, limit).astype(kind)


def setup_inputs(seed: int = 0) -> dict:
    keys = jax.random.split(jax.random.key(seed), 7)
    control = normal_values(keys[0], (MEMBERS, LEV, HX, HY), 1.0, 6.0, ((0, 8), (1, 4)), jnp.float32)
    kappa_table = jnp.clip(jnp.exp(jax.random.uniform(keys[1], (KAPPAS,), jnp.float32, math.log(0.02), math.log(0.24))), 0.02, 0.24)
    kappa_index = plant(jax.random.randint(keys[2], (HX, HY), 0, KAPPAS), jax.random.fold_in(keys[2], 1), 0, KAPPAS - 1).astype(jnp.int32)
    tile_bounds = draw_tile_bounds(jax.random.fold_in(keys[6], 71), 0)
    filter_bands = jnp.clip(jax.random.uniform(keys[4], (TILES, 5, LEV), jnp.float32, -0.3, 0.3), -0.3, 0.3)
    perturbation = heavy_noise(keys[5], (2, MEMBERS, LEV, NCOL), 1.0, 6.0, ((1, 8), (3, 4)), (1, 2, 8, 2.0))
    return {"control": control, "kappa_table": kappa_table, "kappa_index": kappa_index, "tile_bounds": tile_bounds, "filter_bands": filter_bands, "perturbation": perturbation}


def neighbours(state):
    east = jnp.concatenate([state[..., 1:, :], state[..., -1:, :]], axis=-2)
    west = jnp.concatenate([state[..., :1, :], state[..., :-1, :]], axis=-2)
    north = jnp.concatenate([state[..., 1:], state[..., -1:]], axis=-1)
    south = jnp.concatenate([state[..., :1], state[..., :-1]], axis=-1)
    return east, west, north, south


def face_weights(kappa_field):
    return tuple(0.5 * (kappa_field + other) for other in neighbours(kappa_field))


def diffuse_step(state, weights):
    east, west, north, south = neighbours(state)
    update = weights[0] * (east - state) + weights[1] * (west - state)
    update = update + weights[2] * (north - state) + weights[3] * (south - state)
    return state + update


def vertical_filter(values, coefficients):
    levels = values.shape[0]
    padded = jnp.pad(values, ((2, 2), (0, 0)))
    result = values
    for offset in range(5):
        result = result + coefficients[offset] * padded[offset:offset + levels]
    return result


def reference(control, kappa_table, kappa_index, tile_bounds, filter_bands, perturbation):
    kappa_field = kappa_table[kappa_index]
    weights = face_weights(kappa_field)
    columns = jnp.arange(HX * HY, dtype=jnp.int32)
    tile_ids = jnp.sum((columns[None, :] >= tile_bounds[1:-1][:, None]).astype(jnp.int32), axis=0).astype(jnp.int32)
    coefficients = jnp.transpose(filter_bands[tile_ids], (1, 2, 0))

    def one_member(member_field):
        state_field = lax.fori_loop(0, ITERS, lambda step, cur: diffuse_step(cur, weights), member_field)
        flattened = state_field.reshape(LEV, HX * HY)
        return vertical_filter(flattened, coefficients).astype(jnp.bfloat16)

    filtered = lax.map(one_member, control)

    def accumulate(running, members_pair):
        member_filtered, member_pert = members_pair
        return running + member_pert.astype(jnp.float32) * member_filtered.astype(jnp.float32)[None], None

    running, unused = lax.scan(accumulate, jnp.zeros((2, LEV, HX * HY), jnp.float32), (filtered, jnp.moveaxis(perturbation, 1, 0)))
    return running
```

```python
import functools

import jax
import jax.numpy as jnp
from jax import lax
from jax.experimental import pallas as pl
from jax.experimental.pallas import tpu as pltpu
from jax.sharding import PartitionSpec as P

ITERS = 10
F32, BF16 = jnp.float32, jnp.bfloat16
LANES = 128


def inner_size(nm):
    q = 1
    while nm % (2 * q) == 0 and (2 * q) ** 2 <= 2 * nm:
        q *= 2
    return q


def kernel(nm, ng, q, ctrl, table_hbm, kidx_hbm, bounds_hbm, bands_hbm, pert_hbm, out,
           table, bounds, C, S, WE, WN, FL, spread, gather, kidx, kf, bands, bandsb, coef, pert,
           PS, PR, B, G, D, FS, FR, XS, XR, OWN, YS, YR,
           loc_sem, ps_sem, pr_sem, gs_sem, gr_sem, as_sem, ar_sem, bs_sem, br_sem):
    mem = lax.axis_index("mem")
    geo = lax.axis_index("geo")
    o = nm // q
    inner = lax.rem(mem, q)
    outer = mem // q
    hx, lev, hy = S.shape
    nvar, levels, cols = pert.shape
    lm = levels // nm
    wide = levels // q
    rows = hx // ng
    nband, tiles, _ = bands.shape
    parts = hy // LANES
    pad = nband // 2
    nc = FS.shape[1]
    cr = rows // nc
    cw = cr * hy
    npc = XS.shape[1]
    backward = geo < ng // 2

    def at_inner(d):
        return {"mem": outer * q + lax.rem(inner + d, q)}

    def at_outer(d):
        return {"mem": lax.rem(outer + d, o) * q + inner}

    barrier = pltpu.get_barrier_semaphore()
    targets = ([at_inner(d) for d in range(1, q)] + [at_outer(d) for d in range(1, o)]
               + [{"geo": lax.rem(geo + d, ng)} for d in range(1, ng)])
    for target in targets:
        pl.semaphore_signal(barrier, inc=1, device_id=target, device_id_type=pl.DeviceIdType.MESH)

    kidx_cp = pltpu.make_async_copy(kidx_hbm, kidx, loc_sem.at[1])
    kidx_cp.start()
    table_cp = pltpu.make_async_copy(table_hbm, table, loc_sem.at[3])
    table_cp.start()
    pert_cp = pltpu.make_async_copy(pert_hbm.at[:, 0], pert, loc_sem.at[0])
    pert_cp.start()
    ctrl_cps = []
    for l in range(lev):
        cp = pltpu.make_async_copy(ctrl.at[0, l], C.at[:, l], loc_sem.at[5 + l])
        cp.start()
        ctrl_cps.append(cp)
    bands_cp = pltpu.make_async_copy(bands_hbm, bands, loc_sem.at[2])
    bands_cp.start()
    bounds_cp = pltpu.make_async_copy(bounds_hbm, bounds, loc_sem.at[4])
    bounds_cp.start()

    left = lax.broadcasted_iota(jnp.int32, (hy, hy), 0)
    right = lax.broadcasted_iota(jnp.int32, (hy, hy), 1)
    spread[...] = jnp.where(left == (right % LANES) * parts + right // LANES, 1.0, 0.0).astype(BF16)
    gather[...] = jnp.where(right == (left % LANES) * parts + left // LANES, 1.0, 0.0).astype(BF16)

    def turned(i, last):
        return jnp.where(backward, last - i, i)

    kidx_cp.wait()
    table_cp.wait()
    index = jnp.dot(kidx[...].astype(F32).astype(BF16), spread[...], preferred_element_type=F32)
    field = jnp.zeros(index.shape, F32)
    for entry in range(table.shape[0]):
        field = jnp.where(index == float(entry), table[entry], field)
    kf[0:hx] = field
    kf[hx:] = jnp.zeros((kf.shape[0] - hx, hy), F32)
    east = 0.5 * (field + kf[1:hx + 1])
    lane = lax.broadcasted_iota(jnp.int32, (hx, LANES), 1)
    cut = [field[:, p * LANES:(p + 1) * LANES] for p in range(parts)]
    norths = [0.5 * (cut[p] + cut[p + 1]) for p in range(parts - 1)]
    last = 0.5 * (cut[-1] + pltpu.roll(cut[0], LANES - 1, axis=1))
    norths.append(jnp.where(lane < LANES - 1, last, 0.0))
    for i in range(hx):
        if i < hx - 1:
            WE[turned(i, hx - 2)] = jnp.broadcast_to(east[i:i + 1], (lev, hy))
        to = turned(i, hx - 1)
        for p in range(parts):
            WN[to, :, p * LANES:(p + 1) * LANES] = jnp.broadcast_to(norths[p][i:i + 1], (lev, LANES))

    def piece(vals, i):
        return jnp.concatenate([v[(k * q + i) * lm:(k * q + i + 1) * lm] for v in vals for k in range(o)], axis=0)

    def strip(k):
        return pl.ds(pl.multiple_of(k * hy, LANES), hy)

    pert_cp.wait()
    for c in range(npc, nc):
        def repack(r, carry, c=c):
            at = strip(c * cr + r)
            vals = [pert[v, :, at].astype(F32) for v in range(nvar)]
            for i in range(q):
                PS[i, c - npc, :, strip(r)] = piece(vals, i).astype(BF16)
            return carry

        lax.fori_loop(0, cr, repack, 0)
    pl.semaphore_wait(barrier, len(targets))

    def inner_copy(src, dst, send, recv, c, k, d):
        return pltpu.make_async_remote_copy(
            src_ref=src.at[lax.rem(inner + d, q), k], dst_ref=dst.at[d, k], send_sem=send.at[d, c], recv_sem=recv.at[d, c],
            device_id=at_inner(d), device_id_type=pl.DeviceIdType.MESH)

    pert_ex = [[inner_copy(PS, PR, ps_sem, pr_sem, c, c - npc, d) for d in range(1, q)] for c in range(npc, nc)]
    for cps in pert_ex:
        for cp in cps:
            cp.start()

    for cp in ctrl_cps:
        cp.wait()
    group = rows if (rows * lev) % 8 == 0 else hx
    for i in range(0, hx, group):
        x = C[i:i + group].reshape(group * lev, hy)
        high = x.astype(BF16)
        low = (x - high.astype(F32)).astype(BF16)
        x = (jnp.dot(high, spread[...], preferred_element_type=F32)
             + jnp.dot(low, spread[...], preferred_element_type=F32))
        x = x.reshape(group, lev, hy)
        for r in range(group):
            S[turned(i + r, hx - 1)] = x[r]

    def row_of(ref, i):
        return [ref[i, :, p * LANES:(p + 1) * LANES] for p in range(parts)]

    def sweep(it, lo, count, first, final):
        s = row_of(S, lo)
        before = None if first else row_of(FL, it)
        for j in range(count):
            i = lo + j
            wn = row_of(WN, i)
            ahead = s[1:] + [pltpu.roll(s[0], LANES - 1, axis=1)]
            flux = [wn[p] * (ahead[p] - s[p]) for p in range(parts)]
            behind = [pltpu.roll(flux[-1], 1, axis=1)] + flux[:-1]
            new = [s[p] + (flux[p] - behind[p]) for p in range(parts)]
            if before is not None:
                new = [new[p] - before[p] for p in range(parts)]
            if not (final and j == count - 1):
                after = row_of(S, i + 1)
                we = row_of(WE, i)
                before = [we[p] * (after[p] - s[p]) for p in range(parts)]
                new = [new[p] + before[p] for p in range(parts)]
                s = after
            for p in range(parts):
                S[i, :, p * LANES:(p + 1) * LANES] = new[p]
        if not final:
            for p in range(parts):
                FL[it, :, p * LANES:(p + 1) * LANES] = before[p]

    geo_all = []
    for b in range(ng):
        for it in range(ITERS):
            ahead = ITERS - 1 - it
            lo = 0 if b == 0 else min(hx, rows * b + ahead)
            hi = min(hx, rows * (b + 1) + ahead)
            if hi > lo:
                sweep(it, lo, hi - lo, lo == 0, hi == hx)
        band = turned(b, ng - 1)
        if (rows * lev) % 8 == 0:
            x = S[b * rows:(b + 1) * rows].reshape(rows * lev, hy).astype(BF16)
            x = jnp.dot(x, gather[...], preferred_element_type=F32).reshape(rows, lev, hy).astype(BF16)
        else:
            x = [jnp.dot(S[b * rows + r].astype(BF16), gather[...], preferred_element_type=F32).astype(BF16)
                 for r in range(rows)]
        for r in range(rows):
            B[turned(b * rows + r, hx - 1)] = x[r]
        d = lax.rem(band - geo + ng, ng)
        cps = [pltpu.make_async_remote_copy(
            src_ref=B.at[pl.ds(band * rows + c * cr, cr)], dst_ref=G.at[geo, pl.ds(c * cr, cr)],
            send_sem=gs_sem.at[b, c], recv_sem=gr_sem.at[d, c],
            device_id={"geo": band}, device_id_type=pl.DeviceIdType.MESH) for c in range(nc)]
        geo_all.append((band, cps))
        if b < ng // 2:
            for cp in cps:
                cp.start()
        else:
            @pl.when(band != geo)
            def _(cps=cps):
                for cp in cps:
                    cp.start()

    own_geo = [pltpu.make_async_copy(B.at[pl.ds(geo * rows + c * cr, cr)], G.at[geo, pl.ds(c * cr, cr)], gr_sem.at[0, c])
               for c in range(nc)]
    for cp in own_geo:
        cp.start()

    bands_cp.wait()
    bounds_cp.wait()
    eye = (lax.broadcasted_iota(jnp.int32, (levels, levels), 0)
           == lax.broadcasted_iota(jnp.int32, (levels, levels), 1))
    for t in range(tiles):
        for k in range(nband):
            row = jnp.broadcast_to(bands[k, t:t + 1, :], (levels, levels))
            column = jnp.sum(jnp.where(eye, row, 0.0), axis=1, keepdims=True)
            bandsb[t, k] = jnp.broadcast_to(column, (levels, LANES))

    def coefficients(k, carry):
        at = pl.ds(pl.multiple_of(k * LANES, LANES), LANES)
        column = geo * cols + k * LANES + lax.broadcasted_iota(jnp.int32, (levels, LANES), 1)
        past = [column >= bounds[t] for t in range(1, tiles)]
        for k in range(nband):
            value = bandsb[0, k]
            for t in range(1, tiles):
                value = jnp.where(past[t - 1], bandsb[t, k], value)
            coef[k, :, at] = value
        return carry

    lax.fori_loop(0, cols // LANES, coefficients, 0)
    base = 8
    D[0:base, :] = jnp.zeros((base, cols), F32)
    D[base + levels:, :] = jnp.zeros((D.shape[0] - base - levels, cols), F32)

    def filtered(k):
        at = strip(k)
        value = D[base:base + levels, at]
        for n in range(nband):
            value = value + coef[n, :, at] * D[base + n - pad:base + n - pad + levels, at]
        return value.astype(BF16).astype(F32), at

    def arrived(d, c):
        return pltpu.make_async_remote_copy(
            src_ref=B.at[pl.ds(c * cr, cr)], dst_ref=G.at[0, pl.ds(c * cr, cr)],
            send_sem=gs_sem.at[0, c], recv_sem=gr_sem.at[d, c],
            device_id={"geo": lax.rem(geo + d, ng)}, device_id_type=pl.DeviceIdType.MESH)

    filt_ex = []
    for c in range(nc):
        own_geo[c].wait()
        for d in range(1, ng):
            arrived(d, c).wait_recv()

        def vertical(r, carry, c=c):
            k = c * cr + r
            for g in range(ng):
                D[base + g * lev:base + (g + 1) * lev, strip(k)] = G[g, k].astype(F32)
            value, at = filtered(k)
            if c < npc:
                vals = [pert[v, :, at].astype(F32) * value for v in range(nvar)]
                for i in range(q):
                    XS[i, c, :, strip(r)] = piece(vals, i).astype(BF16)
            else:
                for i in range(q):
                    FS[i, c, :, strip(r)] = piece([value], i).astype(BF16)
            return carry

        lax.fori_loop(0, cr, vertical, 0)
        if c < npc:
            cps = [inner_copy(XS, XR, as_sem, ar_sem, c, c, d) for d in range(1, q)]
        else:
            cps = [inner_copy(FS, FR, as_sem, ar_sem, c, c, d) for d in range(1, q)]
        for cp in cps:
            cp.start()
        filt_ex.append(cps)

    outer_ex = []
    for c in range(nc):
        for cp in filt_ex[c]:
            cp.wait_recv()
        if c >= npc:
            for cp in pert_ex[c - npc]:
                cp.wait_recv()

        def total(r, carry, c=c):
            at = strip(r)
            if c < npc:
                acc = XS[inner, c, :, at].astype(F32)
                for d in range(1, q):
                    acc = acc + XR[d, c, :, at].astype(F32)
            else:
                f = FS[inner, c, :, at].astype(F32)
                acc = PS[inner, c - npc, :, at].astype(F32) * jnp.concatenate([f] * nvar, axis=0)
                for d in range(1, q):
                    f = FR[d, c, :, at].astype(F32)
                    acc = acc + PR[d, c - npc, :, at].astype(F32) * jnp.concatenate([f] * nvar, axis=0)
            shares = [jnp.concatenate([acc[v * wide + k * lm:v * wide + (k + 1) * lm] for v in range(nvar)], axis=0)
                      for k in range(o)]
            mine = shares[0]
            for k in range(o):
                YS[k, c, :, at] = shares[k].astype(BF16)
                if k:
                    mine = jnp.where(outer == k, shares[k], mine)
            OWN[c, :, at] = mine
            return carry

        lax.fori_loop(0, cr, total, 0)
        cps = [pltpu.make_async_remote_copy(
            src_ref=YS.at[lax.rem(outer + d, o), c], dst_ref=YR.at[d, c], send_sem=bs_sem.at[d, c], recv_sem=br_sem.at[d, c],
            device_id=at_outer(d), device_id_type=pl.DeviceIdType.MESH) for d in range(1, o)]
        for cp in cps:
            cp.start()
        outer_ex.append(cps)

    for c in range(nc):
        for cp in outer_ex[c]:
            cp.wait_recv()

        def finish(r, carry, c=c):
            at = strip(r)
            acc = OWN[c, :, at]
            for d in range(1, o):
                acc = acc + YR[d, c, :, at].astype(F32)
            for v in range(nvar):
                out[v, :, strip(c * cr + r)] = acc[v * lm:(v + 1) * lm]
            return carry

        lax.fori_loop(0, cr, finish, 0)

    for cps in pert_ex + filt_ex + outer_ex:
        for cp in cps:
            cp.wait_send()
    for b, (band, cps) in enumerate(geo_all):
        if b < ng // 2:
            for cp in cps:
                cp.wait_send()
        else:
            @pl.when(band != geo)
            def _(cps=cps):
                for cp in cps:
                    cp.wait_send()


def body(nm, ng, control, kappa_table, kappa_index, tile_bounds, filter_bands, perturbation):
    _, lev, hx, hy = control.shape
    nvar, _, levels, cols = perturbation.shape
    lm = levels // nm
    rows = hx // ng
    tiles, nband, _ = filter_bands.shape
    q = inner_size(nm)
    o = nm // q
    wide = levels // q
    cr = max(1, rows // 4)
    nc = rows // cr
    npc = 1
    cw = cr * hy
    dma = pltpu.SemaphoreType.DMA
    hbm = pl.BlockSpec(memory_space=pl.ANY)
    return pl.pallas_call(
        functools.partial(kernel, nm, ng, q),
        out_shape=jax.ShapeDtypeStruct((nvar, lm, cols), F32),
        in_specs=[hbm] * 6,
        out_specs=pl.BlockSpec(memory_space=pltpu.VMEM),
        scratch_shapes=[
            pltpu.SMEM(kappa_table.shape, F32),
            pltpu.SMEM(tile_bounds.shape, jnp.int32),
            pltpu.VMEM((hx, lev, hy), F32),
            pltpu.VMEM((hx, lev, hy), F32),
            pltpu.VMEM((hx, lev, hy), F32),
            pltpu.VMEM((hx, lev, hy), F32),
            pltpu.VMEM((ITERS, lev, hy), F32),
            pltpu.VMEM((hy, hy), BF16),
            pltpu.VMEM((hy, hy), BF16),
            pltpu.VMEM((hx, hy), jnp.int32),
            pltpu.VMEM((hx + 8, hy), F32),
            pltpu.VMEM((nband, tiles, levels), F32),
            pltpu.VMEM((tiles, nband, levels, LANES), F32),
            pltpu.VMEM((nband, levels, cols), F32),
            pltpu.VMEM((nvar, levels, cols), BF16),
            pltpu.VMEM((q, nc - npc, nvar * wide, cw), BF16),
            pltpu.VMEM((q, nc - npc, nvar * wide, cw), BF16),
            pltpu.VMEM((hx, lev, hy), BF16),
            pltpu.VMEM((ng, rows, lev, hy), BF16),
            pltpu.VMEM((levels + 16, cols), F32),
            pltpu.VMEM((q, nc, wide, cw), BF16),
            pltpu.VMEM((q, nc, wide, cw), BF16),
            pltpu.VMEM((q, npc, nvar * wide, cw), BF16),
            pltpu.VMEM((q, npc, nvar * wide, cw), BF16),
            pltpu.VMEM((nc, nvar * lm, cw), F32),
            pltpu.VMEM((o, nc, nvar * lm, cw), BF16),
            pltpu.VMEM((o, nc, nvar * lm, cw), BF16),
            dma((5 + lev,)), dma((q, nc)), dma((q, nc)), dma((ng, nc)), dma((ng, nc)),
            dma((q, nc)), dma((q, nc)), dma((o, nc)), dma((o, nc)),
        ],
        compiler_params=pltpu.CompilerParams(
            collective_id=0, has_side_effects=True, vmem_limit_bytes=56 * 2**20),
    )(control, kappa_table, kappa_index, tile_bounds, jnp.swapaxes(filter_bands, 0, 1), perturbation)


def solution(mesh):
    in_specs = (P("mem", "geo", None, None), P(), P(), P(), P(), P(None, "mem", None, "geo"))
    out_specs = P(None, "mem", "geo")
    run = functools.partial(body, mesh.shape["mem"], mesh.shape["geo"])
    return jax.shard_map(run, mesh=mesh, in_specs=in_specs, out_specs=out_specs, check_vma=False)
```

```python
import functools

import jax
import jax.numpy as jnp
from jax import lax
from jax.experimental import pallas as pl
from jax.experimental.pallas import tpu as pltpu
from jax.sharding import PartitionSpec as P

ITERS = 10
F32, BF16 = jnp.float32, jnp.bfloat16
LANES = 128


def inner_size(nm):
    q = 1
    while nm % (2 * q) == 0 and (2 * q) ** 2 <= 2 * nm:
        q *= 2
    return q


def kernel(nm, ng, q, ctrl, table_hbm, kidx_hbm, bounds_hbm, bands_hbm, pert_hbm, out,
           table, bounds, C, S, WE, WN, WS, FL, spread, gather, kidx, kf, bands, bandsb, coef, pert,
           PS, PR, B, G, D, FS, FR, XS, XR, OWN, YS, YR,
           loc_sem, ps_sem, pr_sem, gs_sem, gr_sem, as_sem, ar_sem, bs_sem, br_sem):
    mem = lax.axis_index("mem")
    geo = lax.axis_index("geo")
    o = nm // q
    inner = lax.rem(mem, q)
    outer = mem // q
    hx, lev, hy = S.shape
    nvar, levels, cols = pert.shape
    lm = levels // nm
    wide = levels // q
    rows = hx // ng
    nband, tiles, _ = bands.shape
    parts = hy // LANES
    pad = nband // 2
    nc = FS.shape[1]
    cr = rows // nc
    cw = cr * hy
    npc = XS.shape[1]
    backward = geo < ng // 2

    def at_inner(d):
        return {"mem": outer * q + lax.rem(inner + d, q)}

    def at_outer(d):
        return {"mem": lax.rem(outer + d, o) * q + inner}

    barrier = pltpu.get_barrier_semaphore()
    targets = ([at_inner(d) for d in range(1, q)] + [at_outer(d) for d in range(1, o)]
               + [{"geo": lax.rem(geo + d, ng)} for d in range(1, ng)])
    for target in targets:
        pl.semaphore_signal(barrier, inc=1, device_id=target, device_id_type=pl.DeviceIdType.MESH)

    kidx_cp = pltpu.make_async_copy(kidx_hbm, kidx, loc_sem.at[1])
    kidx_cp.start()
    table_cp = pltpu.make_async_copy(table_hbm, table, loc_sem.at[3])
    table_cp.start()
    pert_cp = pltpu.make_async_copy(pert_hbm.at[:, 0], pert, loc_sem.at[0])
    pert_cp.start()
    ctrl_cps = []
    for l in range(lev):
        cp = pltpu.make_async_copy(ctrl.at[0, l], C.at[:, l], loc_sem.at[5 + l])
        cp.start()
        ctrl_cps.append(cp)
    bands_cp = pltpu.make_async_copy(bands_hbm, bands, loc_sem.at[2])
    bands_cp.start()
    bounds_cp = pltpu.make_async_copy(bounds_hbm, bounds, loc_sem.at[4])
    bounds_cp.start()

    left = lax.broadcasted_iota(jnp.int32, (hy, hy), 0)
    right = lax.broadcasted_iota(jnp.int32, (hy, hy), 1)
    spread[...] = jnp.where(left == (right % LANES) * parts + right // LANES, 1.0, 0.0).astype(BF16)
    gather[...] = jnp.where(right == (left % LANES) * parts + left // LANES, 1.0, 0.0).astype(BF16)

    def turned(i, last):
        return jnp.where(backward, last - i, i)

    kidx_cp.wait()
    table_cp.wait()
    index = jnp.dot(kidx[...].astype(F32).astype(BF16), spread[...], preferred_element_type=F32)
    field = jnp.zeros(index.shape, F32)
    for entry in range(table.shape[0]):
        field = jnp.where(index == float(entry), table[entry], field)
    kf[0:hx] = field
    kf[hx:] = jnp.zeros((kf.shape[0] - hx, hy), F32)
    east = 0.5 * (field + kf[1:hx + 1])
    lane = lax.broadcasted_iota(jnp.int32, (hx, LANES), 1)
    cut = [field[:, p * LANES:(p + 1) * LANES] for p in range(parts)]
    norths = [0.5 * (cut[p] + cut[p + 1]) for p in range(parts - 1)]
    last = 0.5 * (cut[-1] + pltpu.roll(cut[0], LANES - 1, axis=1))
    norths.append(jnp.where(lane < LANES - 1, last, 0.0))
    south = pltpu.roll(norths[-1], 1, axis=1)
    for i in range(hx):
        if i < hx - 1:
            WE[turned(i, hx - 2)] = jnp.broadcast_to(east[i:i + 1], (lev, hy))
        to = turned(i, hx - 1)
        for p in range(parts):
            WN[to, :, p * LANES:(p + 1) * LANES] = jnp.broadcast_to(norths[p][i:i + 1], (lev, LANES))
        WS[to] = jnp.broadcast_to(south[i:i + 1], (lev, LANES))

    def piece(vals, i):
        return jnp.concatenate([v[(k * q + i) * lm:(k * q + i + 1) * lm] for v in vals for k in range(o)], axis=0)

    def strip(k):
        return pl.ds(pl.multiple_of(k * hy, LANES), hy)

    pert_cp.wait()
    for c in range(npc, nc):
        def repack(r, carry, c=c):
            at = strip(c * cr + r)
            vals = [pert[v, :, at].astype(F32) for v in range(nvar)]
            for i in range(q):
                PS[i, c - npc, :, strip(r)] = piece(vals, i).astype(BF16)
            return carry

        lax.fori_loop(0, cr, repack, 0)
    pl.semaphore_wait(barrier, len(targets))

    def inner_copy(src, dst, send, recv, c, k, d):
        return pltpu.make_async_remote_copy(
            src_ref=src.at[lax.rem(inner + d, q), k], dst_ref=dst.at[d, k], send_sem=send.at[d, c], recv_sem=recv.at[d, c],
            device_id=at_inner(d), device_id_type=pl.DeviceIdType.MESH)

    pert_ex = [[inner_copy(PS, PR, ps_sem, pr_sem, c, c - npc, d) for d in range(1, q)] for c in range(npc, nc)]
    for cps in pert_ex:
        for cp in cps:
            cp.start()

    for cp in ctrl_cps:
        cp.wait()
    group = rows if (rows * lev) % 8 == 0 else hx
    for i in range(0, hx, group):
        x = C[i:i + group].reshape(group * lev, hy)
        high = x.astype(BF16)
        low = (x - high.astype(F32)).astype(BF16)
        x = (jnp.dot(high, spread[...], preferred_element_type=F32)
             + jnp.dot(low, spread[...], preferred_element_type=F32))
        x = x.reshape(group, lev, hy)
        for r in range(group):
            S[turned(i + r, hx - 1)] = x[r]

    def row_of(ref, i):
        return [ref[i, :, p * LANES:(p + 1) * LANES] for p in range(parts)]

    def sweep(it, lo, hi):
        s = row_of(S, lo)
        before = row_of(FL, it) if lo else None
        for i in range(lo, hi):
            wn = row_of(WN, i)
            ahead = s[1:] + [pltpu.roll(s[0], LANES - 1, axis=1)]
            flux = [wn[p] * (ahead[p] - s[p]) for p in range(parts)]
            behind = [WS[i] * (s[0] - pltpu.roll(s[-1], 1, axis=1))] + flux[:-1]
            new = [s[p] + (flux[p] - behind[p]) for p in range(parts)]
            if before is not None:
                new = [new[p] - before[p] for p in range(parts)]
            if i < hx - 1:
                after = row_of(S, i + 1)
                we = row_of(WE, i)
                before = [we[p] * (after[p] - s[p]) for p in range(parts)]
                new = [new[p] + before[p] for p in range(parts)]
                s = after
            for p in range(parts):
                S[i, :, p * LANES:(p + 1) * LANES] = new[p]
        if hi < hx:
            for p in range(parts):
                FL[it, :, p * LANES:(p + 1) * LANES] = before[p]

    half = ng // 2
    span = half * rows
    geo_all = []
    for b in range(2):
        for it in range(ITERS):
            lo, hi = (0, min(hx, span + ITERS - 1 - it)) if b == 0 else (min(hx, span + ITERS - 1 - it), hx)
            if hi > lo:
                sweep(it, lo, hi)
        if (span * lev) % 8 == 0:
            x = S[b * span:(b + 1) * span].reshape(span * lev, hy).astype(BF16)
            x = jnp.dot(x, gather[...], preferred_element_type=F32).reshape(span, lev, hy).astype(BF16)
        else:
            x = [jnp.dot(S[b * span + r].astype(BF16), gather[...], preferred_element_type=F32).astype(BF16)
                 for r in range(span)]
        for r in range(span):
            B[turned(b * span + r, hx - 1)] = x[r]
        for j in range(half):
            band = j + jnp.where(backward, half, 0) if b == 0 else j + jnp.where(backward, 0, half)
            d = lax.rem(band - geo + ng, ng)
            cps = [pltpu.make_async_remote_copy(
                src_ref=B.at[pl.ds(band * rows + c * cr, cr)], dst_ref=G.at[geo, pl.ds(c * cr, cr)],
                send_sem=gs_sem.at[b * half + j, c], recv_sem=gr_sem.at[d, c],
                device_id={"geo": band}, device_id_type=pl.DeviceIdType.MESH) for c in range(nc)]
            geo_all.append((b, band, cps))
            if b == 0:
                for cp in cps:
                    cp.start()
            else:
                @pl.when(band != geo)
                def _(cps=cps):
                    for cp in cps:
                        cp.start()

    own_geo = [pltpu.make_async_copy(B.at[pl.ds(geo * rows + c * cr, cr)], G.at[geo, pl.ds(c * cr, cr)], gr_sem.at[0, c])
               for c in range(nc)]
    for cp in own_geo:
        cp.start()

    bands_cp.wait()
    bounds_cp.wait()
    eye = (lax.broadcasted_iota(jnp.int32, (levels, levels), 0)
           == lax.broadcasted_iota(jnp.int32, (levels, levels), 1))
    for t in range(tiles):
        for k in range(nband):
            row = jnp.broadcast_to(bands[k, t:t + 1, :], (levels, levels))
            column = jnp.sum(jnp.where(eye, row, 0.0), axis=1, keepdims=True)
            bandsb[t, k] = jnp.broadcast_to(column, (levels, LANES))

    def coefficients(k, carry):
        at = pl.ds(pl.multiple_of(k * LANES, LANES), LANES)
        column = geo * cols + k * LANES + lax.broadcasted_iota(jnp.int32, (levels, LANES), 1)
        past = [column >= bounds[t] for t in range(1, tiles)]
        for k in range(nband):
            value = bandsb[0, k]
            for t in range(1, tiles):
                value = jnp.where(past[t - 1], bandsb[t, k], value)
            coef[k, :, at] = value
        return carry

    lax.fori_loop(0, cols // LANES, coefficients, 0)
    base = 8
    D[0:base, :] = jnp.zeros((base, cols), F32)
    D[base + levels:, :] = jnp.zeros((D.shape[0] - base - levels, cols), F32)

    def filtered(k):
        at = strip(k)
        value = D[base:base + levels, at]
        for n in range(nband):
            value = value + coef[n, :, at] * D[base + n - pad:base + n - pad + levels, at]
        return value.astype(BF16).astype(F32), at

    def arrived(d, c):
        return pltpu.make_async_remote_copy(
            src_ref=B.at[pl.ds(c * cr, cr)], dst_ref=G.at[0, pl.ds(c * cr, cr)],
            send_sem=gs_sem.at[0, c], recv_sem=gr_sem.at[d, c],
            device_id={"geo": lax.rem(geo + d, ng)}, device_id_type=pl.DeviceIdType.MESH)

    filt_ex = []
    for c in range(nc):
        own_geo[c].wait()
        for d in range(1, ng):
            arrived(d, c).wait_recv()

        def vertical(r, carry, c=c):
            k = c * cr + r
            for g in range(ng):
                D[base + g * lev:base + (g + 1) * lev, strip(k)] = G[g, k].astype(F32)
            value, at = filtered(k)
            if c < npc:
                vals = [pert[v, :, at].astype(F32) * value for v in range(nvar)]
                for i in range(q):
                    XS[i, c, :, strip(r)] = piece(vals, i).astype(BF16)
            else:
                for i in range(q):
                    FS[i, c, :, strip(r)] = piece([value], i).astype(BF16)
            return carry

        lax.fori_loop(0, cr, vertical, 0)
        if c < npc:
            cps = [inner_copy(XS, XR, as_sem, ar_sem, c, c, d) for d in range(1, q)]
        else:
            cps = [inner_copy(FS, FR, as_sem, ar_sem, c, c, d) for d in range(1, q)]
        for cp in cps:
            cp.start()
        filt_ex.append(cps)

    outer_ex = []
    for c in range(nc):
        for cp in filt_ex[c]:
            cp.wait_recv()
        if c >= npc:
            for cp in pert_ex[c - npc]:
                cp.wait_recv()

        def total(r, carry, c=c):
            at = strip(r)
            if c < npc:
                acc = XS[inner, c, :, at].astype(F32)
                for d in range(1, q):
                    acc = acc + XR[d, c, :, at].astype(F32)
            else:
                f = FS[inner, c, :, at].astype(F32)
                acc = PS[inner, c - npc, :, at].astype(F32) * jnp.concatenate([f] * nvar, axis=0)
                for d in range(1, q):
                    f = FR[d, c, :, at].astype(F32)
                    acc = acc + PR[d, c - npc, :, at].astype(F32) * jnp.concatenate([f] * nvar, axis=0)
            shares = [jnp.concatenate([acc[v * wide + k * lm:v * wide + (k + 1) * lm] for v in range(nvar)], axis=0)
                      for k in range(o)]
            mine = shares[0]
            for k in range(o):
                YS[k, c, :, at] = shares[k].astype(BF16)
                if k:
                    mine = jnp.where(outer == k, shares[k], mine)
            OWN[c, :, at] = mine
            return carry

        lax.fori_loop(0, cr, total, 0)
        cps = [pltpu.make_async_remote_copy(
            src_ref=YS.at[lax.rem(outer + d, o), c], dst_ref=YR.at[d, c], send_sem=bs_sem.at[d, c], recv_sem=br_sem.at[d, c],
            device_id=at_outer(d), device_id_type=pl.DeviceIdType.MESH) for d in range(1, o)]
        for cp in cps:
            cp.start()
        outer_ex.append(cps)

    for c in range(nc):
        for cp in outer_ex[c]:
            cp.wait_recv()

        def finish(r, carry, c=c):
            at = strip(r)
            acc = OWN[c, :, at]
            for d in range(1, o):
                acc = acc + YR[d, c, :, at].astype(F32)
            for v in range(nvar):
                out[v, :, strip(c * cr + r)] = acc[v * lm:(v + 1) * lm]
            return carry

        lax.fori_loop(0, cr, finish, 0)

    for cps in pert_ex + filt_ex + outer_ex:
        for cp in cps:
            cp.wait_send()
    for b, band, cps in geo_all:
        if b == 0:
            for cp in cps:
                cp.wait_send()
        else:
            @pl.when(band != geo)
            def _(cps=cps):
                for cp in cps:
                    cp.wait_send()


def body(nm, ng, control, kappa_table, kappa_index, tile_bounds, filter_bands, perturbation):
    _, lev, hx, hy = control.shape
    nvar, _, levels, cols = perturbation.shape
    lm = levels // nm
    rows = hx // ng
    tiles, nband, _ = filter_bands.shape
    q = inner_size(nm)
    o = nm // q
    wide = levels // q
    cr = max(1, rows // 4)
    nc = rows // cr
    npc = 1
    cw = cr * hy
    dma = pltpu.SemaphoreType.DMA
    hbm = pl.BlockSpec(memory_space=pl.ANY)
    return pl.pallas_call(
        functools.partial(kernel, nm, ng, q),
        out_shape=jax.ShapeDtypeStruct((nvar, lm, cols), F32),
        in_specs=[hbm] * 6,
        out_specs=pl.BlockSpec(memory_space=pltpu.VMEM),
        scratch_shapes=[
            pltpu.SMEM(kappa_table.shape, F32),
            pltpu.SMEM(tile_bounds.shape, jnp.int32),
            pltpu.VMEM((hx, lev, hy), F32),
            pltpu.VMEM((hx, lev, hy), F32),
            pltpu.VMEM((hx, lev, hy), F32),
            pltpu.VMEM((hx, lev, hy), F32),
            pltpu.VMEM((hx, lev, LANES), F32),
            pltpu.VMEM((ITERS, lev, hy), F32),
            pltpu.VMEM((hy, hy), BF16),
            pltpu.VMEM((hy, hy), BF16),
            pltpu.VMEM((hx, hy), jnp.int32),
            pltpu.VMEM((hx + 8, hy), F32),
            pltpu.VMEM((nband, tiles, levels), F32),
            pltpu.VMEM((tiles, nband, levels, LANES), F32),
            pltpu.VMEM((nband, levels, cols), F32),
            pltpu.VMEM((nvar, levels, cols), BF16),
            pltpu.VMEM((q, nc - npc, nvar * wide, cw), BF16),
            pltpu.VMEM((q, nc - npc, nvar * wide, cw), BF16),
            pltpu.VMEM((hx, lev, hy), BF16),
            pltpu.VMEM((ng, rows, lev, hy), BF16),
            pltpu.VMEM((levels + 16, cols), F32),
            pltpu.VMEM((q, nc, wide, cw), BF16),
            pltpu.VMEM((q, nc, wide, cw), BF16),
            pltpu.VMEM((q, npc, nvar * wide, cw), BF16),
            pltpu.VMEM((q, npc, nvar * wide, cw), BF16),
            pltpu.VMEM((nc, nvar * lm, cw), F32),
            pltpu.VMEM((o, nc, nvar * lm, cw), BF16),
            pltpu.VMEM((o, nc, nvar * lm, cw), BF16),
            dma((5 + lev,)), dma((q, nc)), dma((q, nc)), dma((ng, nc)), dma((ng, nc)),
            dma((q, nc)), dma((q, nc)), dma((o, nc)), dma((o, nc)),
        ],
        compiler_params=pltpu.CompilerParams(
            collective_id=0, has_side_effects=True, vmem_limit_bytes=56 * 2**20),
    )(control, kappa_table, kappa_index, tile_bounds, jnp.swapaxes(filter_bands, 0, 1), perturbation)


def solution(mesh):
    in_specs = (P("mem", "geo", None, None), P(), P(), P(), P(), P(None, "mem", None, "geo"))
    out_specs = P(None, "mem", "geo")
    run = functools.partial(body, mesh.shape["mem"], mesh.shape["geo"])
    return jax.shard_map(run, mesh=mesh, in_specs=in_specs, out_specs=out_specs, check_vma=False)
```

```python
import functools

import jax
import jax.numpy as jnp
from jax import lax
from jax.experimental import pallas as pl
from jax.experimental.pallas import tpu as pltpu
from jax.sharding import PartitionSpec as P

ITERS = 10
F32, BF16 = jnp.float32, jnp.bfloat16
LANES = 128


def inner_size(nm):
    q = 1
    while nm % (2 * q) == 0 and (2 * q) ** 2 <= 2 * nm:
        q *= 2
    return q


def kernel(nm, ng, q, ctrl, table_hbm, kidx_hbm, bounds_hbm, bands_hbm, pert_hbm, out,
           table, bounds, C, S, WE, WN, WS, FL, spread, gather, kidx, kf, bands, bandsb, coef, pert,
           PS, PR, B, G, D, FS, FR, XS, XR, OWN, YS, YR,
           loc_sem, send_sem, pr_sem, gr_sem, ar_sem, br_sem):
    mem = lax.axis_index("mem")
    geo = lax.axis_index("geo")
    o = nm // q
    inner = lax.rem(mem, q)
    outer = mem // q
    hx, lev, hy = S.shape
    nvar, levels, cols = pert.shape
    lm = levels // nm
    wide = levels // q
    rows = hx // ng
    nband, tiles, _ = bands.shape
    parts = hy // LANES
    pad = nband // 2
    nc = OWN.shape[0]
    cr = rows // nc
    cw = cr * hy
    npc = XS.shape[1]
    backward = geo < ng // 2

    def at_inner(d):
        return {"mem": outer * q + lax.rem(inner + d, q)}

    def at_outer(d):
        return {"mem": lax.rem(outer + d, o) * q + inner}

    barrier = pltpu.get_barrier_semaphore()
    targets = ([at_inner(d) for d in range(1, q)] + [at_outer(d) for d in range(1, o)]
               + [{"geo": lax.rem(geo + d, ng)} for d in range(1, ng)])
    for target in targets:
        pl.semaphore_signal(barrier, inc=1, device_id=target, device_id_type=pl.DeviceIdType.MESH)

    def landed(ref, sem):
        pltpu.make_async_copy(ref, ref, sem).wait()

    pert_cp = pltpu.make_async_copy(pert_hbm.at[:, 0], pert, loc_sem.at[0])
    pert_cp.start()
    kidx_cp = pltpu.make_async_copy(kidx_hbm, kidx, loc_sem.at[1])
    kidx_cp.start()
    table_cp = pltpu.make_async_copy(table_hbm, table, loc_sem.at[2])
    table_cp.start()
    for l in range(lev):
        pltpu.make_async_copy(ctrl.at[0, l], C.at[:, l], loc_sem.at[3]).start()
    bands_cp = pltpu.make_async_copy(bands_hbm, bands, loc_sem.at[4])
    bands_cp.start()
    bounds_cp = pltpu.make_async_copy(bounds_hbm, bounds, loc_sem.at[5])
    bounds_cp.start()

    left = lax.broadcasted_iota(jnp.int32, (hy, hy), 0)
    right = lax.broadcasted_iota(jnp.int32, (hy, hy), 1)
    spread[...] = jnp.where(left == (right % LANES) * parts + right // LANES, 1.0, 0.0).astype(BF16)
    gather[...] = jnp.where(right == (left % LANES) * parts + left // LANES, 1.0, 0.0).astype(BF16)

    def piece(vals, i):
        return jnp.concatenate([v[(k * q + i) * lm:(k * q + i + 1) * lm] for v in vals for k in range(o)], axis=0)

    def strip(k):
        return pl.ds(pl.multiple_of(k * hy, LANES), hy)

    pert_cp.wait()
    for c in range(npc, nc):
        def repack(r, carry, c=c):
            at = strip(c * cr + r)
            vals = [pert[v, :, at].astype(F32) for v in range(nvar)]
            for i in range(q):
                PS[i, c - npc, :, strip(r)] = piece(vals, i).astype(BF16)
            return carry

        lax.fori_loop(0, cr, repack, 0)
    pl.semaphore_wait(barrier, len(targets))

    def inner_send(src, dst, k, send, recv):
        for d in range(1, q):
            pltpu.make_async_remote_copy(
                src_ref=src.at[lax.rem(inner + d, q), k], dst_ref=dst.at[d, k], send_sem=send, recv_sem=recv,
                device_id=at_inner(d), device_id_type=pl.DeviceIdType.MESH).start()

    for k in range(nc - npc):
        inner_send(PS, PR, k, send_sem.at[0], pr_sem.at[k])

    def turned(i, last):
        return jnp.where(backward, last - i, i)

    kidx_cp.wait()
    table_cp.wait()
    landed(C, loc_sem.at[3])
    index = jnp.dot(kidx[...].astype(F32).astype(BF16), spread[...], preferred_element_type=F32)
    field = jnp.zeros(index.shape, F32)
    for entry in range(table.shape[0]):
        field = jnp.where(index == float(entry), table[entry], field)
    kf[0:hx] = field
    kf[hx:] = jnp.zeros((kf.shape[0] - hx, hy), F32)
    east = 0.5 * (field + kf[1:hx + 1])
    lane = lax.broadcasted_iota(jnp.int32, (hx, LANES), 1)
    cut = [field[:, p * LANES:(p + 1) * LANES] for p in range(parts)]
    norths = [0.5 * (cut[p] + cut[p + 1]) for p in range(parts - 1)]
    last = 0.5 * (cut[-1] + pltpu.roll(cut[0], LANES - 1, axis=1))
    norths.append(jnp.where(lane < LANES - 1, last, 0.0))
    south = pltpu.roll(norths[-1], 1, axis=1)
    for i in range(hx):
        if i < hx - 1:
            WE[turned(i, hx - 2)] = jnp.broadcast_to(east[i:i + 1], (lev, hy))
        to = turned(i, hx - 1)
        for p in range(parts):
            WN[to, :, p * LANES:(p + 1) * LANES] = jnp.broadcast_to(norths[p][i:i + 1], (lev, LANES))
        WS[to] = jnp.broadcast_to(south[i:i + 1], (lev, LANES))

    group = rows if (rows * lev) % 8 == 0 else hx
    for i in range(0, hx, group):
        x = C[i:i + group].reshape(group * lev, hy)
        high = x.astype(BF16)
        low = (x - high.astype(F32)).astype(BF16)
        x = (jnp.dot(high, spread[...], preferred_element_type=F32)
             + jnp.dot(low, spread[...], preferred_element_type=F32))
        x = x.reshape(group, lev, hy)
        for r in range(group):
            S[turned(i + r, hx - 1)] = x[r]

    def row_of(ref, i):
        return [ref[i, :, p * LANES:(p + 1) * LANES] for p in range(parts)]

    def sweep(it, lo, hi):
        s = row_of(S, lo)
        before = row_of(FL, it) if lo else None
        for i in range(lo, hi):
            wn = row_of(WN, i)
            ahead = s[1:] + [pltpu.roll(s[0], LANES - 1, axis=1)]
            flux = [wn[p] * (ahead[p] - s[p]) for p in range(parts)]
            behind = [WS[i] * (s[0] - pltpu.roll(s[-1], 1, axis=1))] + flux[:-1]
            new = [s[p] + (flux[p] - behind[p]) for p in range(parts)]
            if before is not None:
                new = [new[p] - before[p] for p in range(parts)]
            if i < hx - 1:
                after = row_of(S, i + 1)
                we = row_of(WE, i)
                before = [we[p] * (after[p] - s[p]) for p in range(parts)]
                new = [new[p] + before[p] for p in range(parts)]
                s = after
            for p in range(parts):
                S[i, :, p * LANES:(p + 1) * LANES] = new[p]
        if hi < hx:
            for p in range(parts):
                FL[it, :, p * LANES:(p + 1) * LANES] = before[p]

    half = ng // 2
    span = half * rows
    for b in range(2):
        for it in range(ITERS):
            lo, hi = (0, min(hx, span + ITERS - 1 - it)) if b == 0 else (min(hx, span + ITERS - 1 - it), hx)
            if hi > lo:
                sweep(it, lo, hi)
        if (span * lev) % 8 == 0:
            x = S[b * span:(b + 1) * span].reshape(span * lev, hy).astype(BF16)
            x = jnp.dot(x, gather[...], preferred_element_type=F32).reshape(span, lev, hy).astype(BF16)
        else:
            x = [jnp.dot(S[b * span + r].astype(BF16), gather[...], preferred_element_type=F32).astype(BF16)
                 for r in range(span)]
        for r in range(span):
            B[turned(b * span + r, hx - 1)] = x[r]
        for j in range(half):
            band = j + jnp.where(backward, half, 0) if b == 0 else j + jnp.where(backward, 0, half)
            cps = [pltpu.make_async_remote_copy(
                src_ref=B.at[pl.ds(band * rows + c * cr, cr)], dst_ref=G.at[geo, pl.ds(c * cr, cr)],
                send_sem=send_sem.at[1], recv_sem=gr_sem.at[c],
                device_id={"geo": band}, device_id_type=pl.DeviceIdType.MESH) for c in range(nc)]
            if b == 0:
                for cp in cps:
                    cp.start()
            else:
                @pl.when(band != geo)
                def _(cps=cps):
                    for cp in cps:
                        cp.start()

    for c in range(nc):
        pltpu.make_async_copy(B.at[pl.ds(geo * rows + c * cr, cr)], G.at[geo, pl.ds(c * cr, cr)], gr_sem.at[c]).start()

    bands_cp.wait()
    bounds_cp.wait()
    eye = (lax.broadcasted_iota(jnp.int32, (levels, levels), 0)
           == lax.broadcasted_iota(jnp.int32, (levels, levels), 1))
    for t in range(tiles):
        for k in range(nband):
            row = jnp.broadcast_to(bands[k, t:t + 1, :], (levels, levels))
            column = jnp.sum(jnp.where(eye, row, 0.0), axis=1, keepdims=True)
            bandsb[t, k] = jnp.broadcast_to(column, (levels, LANES))

    def coefficients(k, carry):
        at = pl.ds(pl.multiple_of(k * LANES, LANES), LANES)
        column = geo * cols + k * LANES + lax.broadcasted_iota(jnp.int32, (levels, LANES), 1)
        past = [column >= bounds[t] for t in range(1, tiles)]
        for k in range(nband):
            value = bandsb[0, k]
            for t in range(1, tiles):
                value = jnp.where(past[t - 1], bandsb[t, k], value)
            coef[k, :, at] = value
        return carry

    lax.fori_loop(0, cols // LANES, coefficients, 0)
    base = 8
    D[0:base, :] = jnp.zeros((base, cols), F32)
    D[base + levels:, :] = jnp.zeros((D.shape[0] - base - levels, cols), F32)

    def filtered(k):
        at = strip(k)
        value = D[base:base + levels, at]
        for n in range(nband):
            value = value + coef[n, :, at] * D[base + n - pad:base + n - pad + levels, at]
        return value.astype(BF16).astype(F32), at

    for c in range(nc):
        landed(G.at[:, pl.ds(c * cr, cr)], gr_sem.at[c])

        def vertical(r, carry, c=c):
            k = c * cr + r
            for g in range(ng):
                D[base + g * lev:base + (g + 1) * lev, strip(k)] = G[g, k].astype(F32)
            value, at = filtered(k)
            if c < npc:
                vals = [pert[v, :, at].astype(F32) * value for v in range(nvar)]
                for i in range(q):
                    XS[i, c, :, strip(r)] = piece(vals, i).astype(BF16)
            else:
                for i in range(q):
                    FS[i, c - npc, :, strip(r)] = piece([value], i).astype(BF16)
            return carry

        lax.fori_loop(0, cr, vertical, 0)
        if c < npc:
            inner_send(XS, XR, c, send_sem.at[2], ar_sem.at[c])
        else:
            inner_send(FS, FR, c - npc, send_sem.at[3], ar_sem.at[c])

    others = pl.ds(1, q - 1)
    for c in range(nc):
        if c < npc:
            landed(XR.at[others, c], ar_sem.at[c])
        else:
            landed(FR.at[others, c - npc], ar_sem.at[c])
            landed(PR.at[others, c - npc], pr_sem.at[c - npc])

        def total(r, carry, c=c):
            at = strip(r)
            if c < npc:
                acc = XS[inner, c, :, at].astype(F32)
                for d in range(1, q):
                    acc = acc + XR[d, c, :, at].astype(F32)
            else:
                f = FS[inner, c - npc, :, at].astype(F32)
                acc = PS[inner, c - npc, :, at].astype(F32) * jnp.concatenate([f] * nvar, axis=0)
                for d in range(1, q):
                    f = FR[d, c - npc, :, at].astype(F32)
                    acc = acc + PR[d, c - npc, :, at].astype(F32) * jnp.concatenate([f] * nvar, axis=0)
            shares = [jnp.concatenate([acc[v * wide + k * lm:v * wide + (k + 1) * lm] for v in range(nvar)], axis=0)
                      for k in range(o)]
            mine = shares[0]
            for k in range(o):
                YS[k, c, :, at] = shares[k].astype(BF16)
                if k:
                    mine = jnp.where(outer == k, shares[k], mine)
            OWN[c, :, at] = mine
            return carry

        lax.fori_loop(0, cr, total, 0)
        for d in range(1, o):
            pltpu.make_async_remote_copy(
                src_ref=YS.at[lax.rem(outer + d, o), c], dst_ref=YR.at[d, c], send_sem=send_sem.at[4], recv_sem=br_sem.at[c],
                device_id=at_outer(d), device_id_type=pl.DeviceIdType.MESH).start()

    for c in range(nc):
        landed(YR.at[pl.ds(1, o - 1), c], br_sem.at[c])

        def finish(r, carry, c=c):
            at = strip(r)
            acc = OWN[c, :, at]
            for d in range(1, o):
                acc = acc + YR[d, c, :, at].astype(F32)
            for v in range(nvar):
                out[v, :, strip(c * cr + r)] = acc[v * lm:(v + 1) * lm]
            return carry

        lax.fori_loop(0, cr, finish, 0)

    landed(PS.at[pl.ds(0, q - 1)], send_sem.at[0])
    landed(B.at[pl.ds(0, hx - rows)], send_sem.at[1])
    landed(XS.at[pl.ds(0, q - 1)], send_sem.at[2])
    landed(FS.at[pl.ds(0, q - 1)], send_sem.at[3])
    landed(YS.at[pl.ds(0, o - 1)], send_sem.at[4])


def body(nm, ng, control, kappa_table, kappa_index, tile_bounds, filter_bands, perturbation):
    _, lev, hx, hy = control.shape
    nvar, _, levels, cols = perturbation.shape
    lm = levels // nm
    rows = hx // ng
    tiles, nband, _ = filter_bands.shape
    q = inner_size(nm)
    o = nm // q
    wide = levels // q
    cr = max(1, rows // 4)
    nc = rows // cr
    npc = 1
    cw = cr * hy
    dma = pltpu.SemaphoreType.DMA
    hbm = pl.BlockSpec(memory_space=pl.ANY)
    return pl.pallas_call(
        functools.partial(kernel, nm, ng, q),
        out_shape=pltpu.VMEM((nvar, lm, cols), F32),
        in_specs=[hbm] * 6,
        out_specs=pl.BlockSpec(memory_space=pltpu.VMEM),
        scratch_shapes=[
            pltpu.SMEM(kappa_table.shape, F32),
            pltpu.SMEM(tile_bounds.shape, jnp.int32),
            pltpu.VMEM((hx, lev, hy), F32),
            pltpu.VMEM((hx, lev, hy), F32),
            pltpu.VMEM((hx, lev, hy), F32),
            pltpu.VMEM((hx, lev, hy), F32),
            pltpu.VMEM((hx, lev, LANES), F32),
            pltpu.VMEM((ITERS, lev, hy), F32),
            pltpu.VMEM((hy, hy), BF16),
            pltpu.VMEM((hy, hy), BF16),
            pltpu.VMEM((hx, hy), jnp.int32),
            pltpu.VMEM((hx + 8, hy), F32),
            pltpu.VMEM((nband, tiles, levels), F32),
            pltpu.VMEM((tiles, nband, levels, LANES), F32),
            pltpu.VMEM((nband, levels, cols), F32),
            pltpu.VMEM((nvar, levels, cols), BF16),
            pltpu.VMEM((q, nc - npc, nvar * wide, cw), BF16),
            pltpu.VMEM((q, nc - npc, nvar * wide, cw), BF16),
            pltpu.VMEM((hx, lev, hy), BF16),
            pltpu.VMEM((ng, rows, lev, hy), BF16),
            pltpu.VMEM((levels + 16, cols), F32),
            pltpu.VMEM((q, nc - npc, wide, cw), BF16),
            pltpu.VMEM((q, nc - npc, wide, cw), BF16),
            pltpu.VMEM((q, npc, nvar * wide, cw), BF16),
            pltpu.VMEM((q, npc, nvar * wide, cw), BF16),
            pltpu.VMEM((nc, nvar * lm, cw), F32),
            pltpu.VMEM((o, nc, nvar * lm, cw), BF16),
            pltpu.VMEM((o, nc, nvar * lm, cw), BF16),
            dma((6,)), dma((5,)), dma((nc - npc,)), dma((nc,)), dma((nc,)), dma((nc,)),
        ],
        compiler_params=pltpu.CompilerParams(
            collective_id=0, has_side_effects=True, vmem_limit_bytes=56 * 2**20),
    )(control, kappa_table, kappa_index, tile_bounds, jnp.swapaxes(filter_bands, 0, 1), perturbation)


def solution(mesh):
    in_specs = (P("mem", "geo", None, None), P(), P(), P(), P(), P(None, "mem", None, "geo"))
    out_specs = P(None, "mem", "geo")
    run = functools.partial(body, mesh.shape["mem"], mesh.shape["geo"])
    return jax.shard_map(run, mesh=mesh, in_specs=in_specs, out_specs=out_specs, check_vma=False)
```

```python
import functools

import jax
import jax.numpy as jnp
from jax import lax
from jax.experimental import pallas as pl
from jax.experimental.pallas import tpu as pltpu
from jax.sharding import PartitionSpec as P

ITERS = 10
F32, BF16 = jnp.float32, jnp.bfloat16
LANES = 128


def inner_size(nm):
    q = 1
    while nm % (2 * q) == 0 and (2 * q) ** 2 <= 2 * nm:
        q *= 2
    return q


def kernel(nm, ng, q, ctrl, table_hbm, kidx_hbm, bounds_hbm, bands_hbm, pert_hbm, out,
           table, bounds, C, S, WE, WN, WS, FL, spread, gather, kidx, kf, bands, bandsb, coef, pert,
           PS, PR, B, G, D, FS, FR, XS, XR, OWN, YS, YR,
           loc_sem, send_sem, pr_sem, gr_sem, ar_sem, br_sem):
    mem = lax.axis_index("mem")
    geo = lax.axis_index("geo")
    o = nm // q
    inner = lax.rem(mem, q)
    outer = mem // q
    hx, lev, hy = S.shape
    nvar, levels, cols = pert.shape
    lm = levels // nm
    wide = levels // q
    rows = hx // ng
    nband, tiles, _ = bands.shape
    parts = hy // LANES
    pad = nband // 2
    nc = OWN.shape[0]
    cr = rows // nc
    cw = cr * hy
    npc = XS.shape[1]
    backward = geo < ng // 2
    near = lax.rem(geo, 2) == 1
    far = jnp.logical_not(near)

    def at_inner(d):
        return {"mem": outer * q + lax.rem(inner + d, q)}

    def at_outer(d):
        return {"mem": lax.rem(outer + d, o) * q + inner}

    barrier = pltpu.get_barrier_semaphore()
    targets = ([at_inner(d) for d in range(1, q)] + [at_outer(d) for d in range(1, o)]
               + [{"geo": lax.rem(geo + d, ng)} for d in range(1, ng)])
    for target in targets:
        pl.semaphore_signal(barrier, inc=1, device_id=target, device_id_type=pl.DeviceIdType.MESH)

    def landed(ref, sem):
        pltpu.make_async_copy(ref, ref, sem).wait()

    pert_cp = pltpu.make_async_copy(pert_hbm.at[:, 0], pert, loc_sem.at[0])
    pert_cp.start()
    kidx_cp = pltpu.make_async_copy(kidx_hbm, kidx, loc_sem.at[1])
    kidx_cp.start()
    table_cp = pltpu.make_async_copy(table_hbm, table, loc_sem.at[2])
    table_cp.start()
    for l in range(lev):
        pltpu.make_async_copy(ctrl.at[0, l], C.at[:, l], loc_sem.at[3]).start()
    bands_cp = pltpu.make_async_copy(bands_hbm, bands, loc_sem.at[4])
    bands_cp.start()
    bounds_cp = pltpu.make_async_copy(bounds_hbm, bounds, loc_sem.at[5])
    bounds_cp.start()

    left = lax.broadcasted_iota(jnp.int32, (hy, hy), 0)
    right = lax.broadcasted_iota(jnp.int32, (hy, hy), 1)
    spread[...] = jnp.where(left == (right % LANES) * parts + right // LANES, 1.0, 0.0).astype(BF16)
    gather[...] = jnp.where(right == (left % LANES) * parts + left // LANES, 1.0, 0.0).astype(BF16)

    def piece(vals, i):
        return jnp.concatenate([v[(k * q + i) * lm:(k * q + i + 1) * lm] for v in vals for k in range(o)], axis=0)

    def strip(k):
        return pl.ds(pl.multiple_of(k * hy, LANES), hy)

    pert_cp.wait()
    def repack(c):
        def step(r, carry):
            at = strip(c * cr + r)
            vals = [pert[v, :, at].astype(F32) for v in range(nvar)]
            for i in range(q):
                PS[i, c, :, strip(r)] = piece(vals, i).astype(BF16)
            return carry

        lax.fori_loop(0, cr, step, 0)

    def inner_send(src, dst, c, send, recv):
        for d in range(1, q):
            pltpu.make_async_remote_copy(
                src_ref=src.at[lax.rem(inner + d, q), c], dst_ref=dst.at[d, c], send_sem=send, recv_sem=recv,
                device_id=at_inner(d), device_id_type=pl.DeviceIdType.MESH).start()

    @pl.when(far)
    def _():
        for c in range(npc):
            repack(c)

    for c in range(npc, nc):
        repack(c)
    pl.semaphore_wait(barrier, len(targets))

    @pl.when(far)
    def _():
        for c in range(npc):
            inner_send(PS, PR, c, send_sem.at[5], pr_sem.at[c])

    for c in range(npc, nc):
        inner_send(PS, PR, c, send_sem.at[0], pr_sem.at[c])

    def turned(i, last):
        return jnp.where(backward, last - i, i)

    kidx_cp.wait()
    table_cp.wait()
    landed(C, loc_sem.at[3])
    index = jnp.dot(kidx[...].astype(F32).astype(BF16), spread[...], preferred_element_type=F32)
    field = jnp.zeros(index.shape, F32)
    for entry in range(table.shape[0]):
        field = jnp.where(index == float(entry), table[entry], field)
    kf[0:hx] = field
    kf[hx:] = jnp.zeros((kf.shape[0] - hx, hy), F32)
    east = 0.5 * (field + kf[1:hx + 1])
    lane = lax.broadcasted_iota(jnp.int32, (hx, LANES), 1)
    cut = [field[:, p * LANES:(p + 1) * LANES] for p in range(parts)]
    norths = [0.5 * (cut[p] + cut[p + 1]) for p in range(parts - 1)]
    last = 0.5 * (cut[-1] + pltpu.roll(cut[0], LANES - 1, axis=1))
    norths.append(jnp.where(lane < LANES - 1, last, 0.0))
    south = pltpu.roll(norths[-1], 1, axis=1)
    for i in range(hx):
        if i < hx - 1:
            WE[turned(i, hx - 2)] = jnp.broadcast_to(east[i:i + 1], (lev, hy))
        to = turned(i, hx - 1)
        for p in range(parts):
            WN[to, :, p * LANES:(p + 1) * LANES] = jnp.broadcast_to(norths[p][i:i + 1], (lev, LANES))
        WS[to] = jnp.broadcast_to(south[i:i + 1], (lev, LANES))

    group = rows if (rows * lev) % 8 == 0 else hx
    for i in range(0, hx, group):
        x = C[i:i + group].reshape(group * lev, hy)
        high = x.astype(BF16)
        low = (x - high.astype(F32)).astype(BF16)
        x = (jnp.dot(high, spread[...], preferred_element_type=F32)
             + jnp.dot(low, spread[...], preferred_element_type=F32))
        x = x.reshape(group, lev, hy)
        for r in range(group):
            S[turned(i + r, hx - 1)] = x[r]

    def row_of(ref, i):
        return [ref[i, :, p * LANES:(p + 1) * LANES] for p in range(parts)]

    def sweep(it, lo, hi):
        s = row_of(S, lo)
        before = row_of(FL, it) if lo else None
        for i in range(lo, hi):
            wn = row_of(WN, i)
            ahead = s[1:] + [pltpu.roll(s[0], LANES - 1, axis=1)]
            flux = [wn[p] * (ahead[p] - s[p]) for p in range(parts)]
            behind = [WS[i] * (s[0] - pltpu.roll(s[-1], 1, axis=1))] + flux[:-1]
            new = [s[p] + (flux[p] - behind[p]) for p in range(parts)]
            if before is not None:
                new = [new[p] - before[p] for p in range(parts)]
            if i < hx - 1:
                after = row_of(S, i + 1)
                we = row_of(WE, i)
                before = [we[p] * (after[p] - s[p]) for p in range(parts)]
                new = [new[p] + before[p] for p in range(parts)]
                s = after
            for p in range(parts):
                S[i, :, p * LANES:(p + 1) * LANES] = new[p]
        if hi < hx:
            for p in range(parts):
                FL[it, :, p * LANES:(p + 1) * LANES] = before[p]

    half = ng // 2
    span = half * rows
    for b in range(2):
        for it in range(ITERS):
            lo, hi = (0, min(hx, span + ITERS - 1 - it)) if b == 0 else (min(hx, span + ITERS - 1 - it), hx)
            if hi > lo:
                sweep(it, lo, hi)
        if (span * lev) % 8 == 0:
            x = S[b * span:(b + 1) * span].reshape(span * lev, hy).astype(BF16)
            x = jnp.dot(x, gather[...], preferred_element_type=F32).reshape(span, lev, hy).astype(BF16)
        else:
            x = [jnp.dot(S[b * span + r].astype(BF16), gather[...], preferred_element_type=F32).astype(BF16)
                 for r in range(span)]
        for r in range(span):
            B[turned(b * span + r, hx - 1)] = x[r]
        for j in range(half):
            band = j + jnp.where(backward, half, 0) if b == 0 else j + jnp.where(backward, 0, half)
            cps = [pltpu.make_async_remote_copy(
                src_ref=B.at[pl.ds(band * rows + c * cr, cr)], dst_ref=G.at[geo, pl.ds(c * cr, cr)],
                send_sem=send_sem.at[1], recv_sem=gr_sem.at[c],
                device_id={"geo": band}, device_id_type=pl.DeviceIdType.MESH) for c in range(nc)]
            if b == 0:
                for cp in cps:
                    cp.start()
            else:
                @pl.when(band != geo)
                def _(cps=cps):
                    for cp in cps:
                        cp.start()

    for c in range(nc):
        pltpu.make_async_copy(B.at[pl.ds(geo * rows + c * cr, cr)], G.at[geo, pl.ds(c * cr, cr)], gr_sem.at[c]).start()

    bands_cp.wait()
    bounds_cp.wait()
    eye = (lax.broadcasted_iota(jnp.int32, (levels, levels), 0)
           == lax.broadcasted_iota(jnp.int32, (levels, levels), 1))
    for t in range(tiles):
        for k in range(nband):
            row = jnp.broadcast_to(bands[k, t:t + 1, :], (levels, levels))
            column = jnp.sum(jnp.where(eye, row, 0.0), axis=1, keepdims=True)
            bandsb[t, k] = jnp.broadcast_to(column, (levels, LANES))

    def coefficients(k, carry):
        at = pl.ds(pl.multiple_of(k * LANES, LANES), LANES)
        column = geo * cols + k * LANES + lax.broadcasted_iota(jnp.int32, (levels, LANES), 1)
        past = [column >= bounds[t] for t in range(1, tiles)]
        for k in range(nband):
            value = bandsb[0, k]
            for t in range(1, tiles):
                value = jnp.where(past[t - 1], bandsb[t, k], value)
            coef[k, :, at] = value
        return carry

    lax.fori_loop(0, cols // LANES, coefficients, 0)
    base = 8
    D[0:base, :] = jnp.zeros((base, cols), F32)
    D[base + levels:, :] = jnp.zeros((D.shape[0] - base - levels, cols), F32)

    def filtered(k):
        at = strip(k)
        value = D[base:base + levels, at]
        for n in range(nband):
            value = value + coef[n, :, at] * D[base + n - pad:base + n - pad + levels, at]
        return value.astype(BF16).astype(F32), at

    def vertical(c, products, send):
        def step(r, carry):
            k = c * cr + r
            for g in range(ng):
                D[base + g * lev:base + (g + 1) * lev, strip(k)] = G[g, k].astype(F32)
            value, at = filtered(k)
            if products:
                vals = [pert[v, :, at].astype(F32) * value for v in range(nvar)]
                for i in range(q):
                    XS[i, c, :, strip(r)] = piece(vals, i).astype(BF16)
            else:
                for i in range(q):
                    FS[i, c, :, strip(r)] = piece([value], i).astype(BF16)
            return carry

        lax.fori_loop(0, cr, step, 0)
        if products:
            inner_send(XS, XR, c, send, ar_sem.at[c])
        else:
            inner_send(FS, FR, c, send, ar_sem.at[c])

    for c in range(nc):
        landed(G.at[:, pl.ds(c * cr, cr)], gr_sem.at[c])
        if c < npc:
            pl.when(near)(functools.partial(vertical, c, True, send_sem.at[2]))
            pl.when(far)(functools.partial(vertical, c, False, send_sem.at[6]))
        else:
            vertical(c, False, send_sem.at[3])

    others = pl.ds(1, q - 1)

    def total(c, products):
        if products:
            landed(XR.at[others, c], ar_sem.at[c])
        else:
            landed(FR.at[others, c], ar_sem.at[c])
            landed(PR.at[others, c], pr_sem.at[c])

        def step(r, carry):
            at = strip(r)
            if products:
                acc = XS[inner, c, :, at].astype(F32)
                for d in range(1, q):
                    acc = acc + XR[d, c, :, at].astype(F32)
            else:
                f = FS[inner, c, :, at].astype(F32)
                acc = PS[inner, c, :, at].astype(F32) * jnp.concatenate([f] * nvar, axis=0)
                for d in range(1, q):
                    f = FR[d, c, :, at].astype(F32)
                    acc = acc + PR[d, c, :, at].astype(F32) * jnp.concatenate([f] * nvar, axis=0)
            shares = [jnp.concatenate([acc[v * wide + k * lm:v * wide + (k + 1) * lm] for v in range(nvar)], axis=0)
                      for k in range(o)]
            mine = shares[0]
            for k in range(o):
                YS[k, c, :, at] = shares[k].astype(BF16)
                if k:
                    mine = jnp.where(outer == k, shares[k], mine)
            OWN[c, :, at] = mine
            return carry

        lax.fori_loop(0, cr, step, 0)

    for c in range(nc):
        if c < npc:
            pl.when(near)(functools.partial(total, c, True))
            pl.when(far)(functools.partial(total, c, False))
        else:
            total(c, False)
        for d in range(1, o):
            pltpu.make_async_remote_copy(
                src_ref=YS.at[lax.rem(outer + d, o), c], dst_ref=YR.at[d, c], send_sem=send_sem.at[4], recv_sem=br_sem.at[c],
                device_id=at_outer(d), device_id_type=pl.DeviceIdType.MESH).start()

    for c in range(nc):
        landed(YR.at[pl.ds(1, o - 1), c], br_sem.at[c])

        def finish(r, carry, c=c):
            at = strip(r)
            acc = OWN[c, :, at]
            for d in range(1, o):
                acc = acc + YR[d, c, :, at].astype(F32)
            for v in range(nvar):
                out[v, :, strip(c * cr + r)] = acc[v * lm:(v + 1) * lm]
            return carry

        lax.fori_loop(0, cr, finish, 0)

    peers = pl.ds(0, q - 1)
    landed(PS.at[peers, pl.ds(npc, nc - npc)], send_sem.at[0])
    landed(B.at[pl.ds(0, hx - rows)], send_sem.at[1])
    landed(FS.at[peers, pl.ds(npc, nc - npc)], send_sem.at[3])
    landed(YS.at[pl.ds(0, o - 1)], send_sem.at[4])

    @pl.when(near)
    def _():
        landed(XS.at[peers], send_sem.at[2])

    @pl.when(far)
    def _():
        landed(PS.at[peers, pl.ds(0, npc)], send_sem.at[5])
        landed(FS.at[peers, pl.ds(0, npc)], send_sem.at[6])


def body(nm, ng, control, kappa_table, kappa_index, tile_bounds, filter_bands, perturbation):
    _, lev, hx, hy = control.shape
    nvar, _, levels, cols = perturbation.shape
    lm = levels // nm
    rows = hx // ng
    tiles, nband, _ = filter_bands.shape
    q = inner_size(nm)
    o = nm // q
    wide = levels // q
    cr = max(1, rows // 4)
    nc = rows // cr
    npc = nc // 2
    cw = cr * hy
    dma = pltpu.SemaphoreType.DMA
    hbm = pl.BlockSpec(memory_space=pl.ANY)
    return pl.pallas_call(
        functools.partial(kernel, nm, ng, q),
        out_shape=pltpu.VMEM((nvar, lm, cols), F32),
        in_specs=[hbm] * 6,
        out_specs=pl.BlockSpec(memory_space=pltpu.VMEM),
        scratch_shapes=[
            pltpu.SMEM(kappa_table.shape, F32),
            pltpu.SMEM(tile_bounds.shape, jnp.int32),
            pltpu.VMEM((hx, lev, hy), F32),
            pltpu.VMEM((hx, lev, hy), F32),
            pltpu.VMEM((hx, lev, hy), F32),
            pltpu.VMEM((hx, lev, hy), F32),
            pltpu.VMEM((hx, lev, LANES), F32),
            pltpu.VMEM((ITERS, lev, hy), F32),
            pltpu.VMEM((hy, hy), BF16),
            pltpu.VMEM((hy, hy), BF16),
            pltpu.VMEM((hx, hy), jnp.int32),
            pltpu.VMEM((hx + 8, hy), F32),
            pltpu.VMEM((nband, tiles, levels), F32),
            pltpu.VMEM((tiles, nband, levels, LANES), F32),
            pltpu.VMEM((nband, levels, cols), F32),
            pltpu.VMEM((nvar, levels, cols), BF16),
            pltpu.VMEM((q, nc, nvar * wide, cw), BF16),
            pltpu.VMEM((q, nc, nvar * wide, cw), BF16),
            pltpu.VMEM((hx, lev, hy), BF16),
            pltpu.VMEM((ng, rows, lev, hy), BF16),
            pltpu.VMEM((levels + 16, cols), F32),
            pltpu.VMEM((q, nc, wide, cw), BF16),
            pltpu.VMEM((q, nc, wide, cw), BF16),
            pltpu.VMEM((q, npc, nvar * wide, cw), BF16),
            pltpu.VMEM((q, npc, nvar * wide, cw), BF16),
            pltpu.VMEM((nc, nvar * lm, cw), F32),
            pltpu.VMEM((o, nc, nvar * lm, cw), BF16),
            pltpu.VMEM((o, nc, nvar * lm, cw), BF16),
            dma((6,)), dma((7,)), dma((nc,)), dma((nc,)), dma((nc,)), dma((nc,)),
        ],
        compiler_params=pltpu.CompilerParams(
            collective_id=0, has_side_effects=True, vmem_limit_bytes=56 * 2**20),
    )(control, kappa_table, kappa_index, tile_bounds, jnp.swapaxes(filter_bands, 0, 1), perturbation)


def solution(mesh):
    in_specs = (P("mem", "geo", None, None), P(), P(), P(), P(), P(None, "mem", None, "geo"))
    out_specs = P(None, "mem", "geo")
    run = functools.partial(body, mesh.shape["mem"], mesh.shape["geo"])
    return jax.shard_map(run, mesh=mesh, in_specs=in_specs, out_specs=out_specs, check_vma=False)
```

```python
import functools

import jax
import jax.numpy as jnp
from jax import lax
from jax.experimental import pallas as pl
from jax.experimental.pallas import tpu as pltpu
from jax.sharding import PartitionSpec as P

ITERS = 10
F32, BF16 = jnp.float32, jnp.bfloat16
LANES = 128


def inner_size(nm):
    q = 1
    while nm % (2 * q) == 0 and (2 * q) ** 2 <= 2 * nm:
        q *= 2
    return q


def kernel(nm, ng, q, ctrl, table_hbm, kidx_hbm, bounds_hbm, bands_hbm, pert_hbm, out,
           table, bounds, C, S, WE, WN, WS, FL, spread, gather, kidx, kf, bands, bandsb, coef, pert,
           PS, PR, B, G, D, FS, FR, XS, XR, OWN, YS, YR,
           loc_sem, pert_sem, send_sem, pr_sem, gr_sem, ar_sem, br_sem):
    mem = lax.axis_index("mem")
    geo = lax.axis_index("geo")
    o = nm // q
    inner = lax.rem(mem, q)
    outer = mem // q
    hx, lev, hy = S.shape
    nvar, levels, cols = pert.shape
    lm = levels // nm
    wide = levels // q
    rows = hx // ng
    nband, tiles, _ = bands.shape
    parts = hy // LANES
    pad = nband // 2
    nc = OWN.shape[0]
    cr = rows // nc
    cw = cr * hy
    npc = XS.shape[1]
    backward = geo < ng // 2
    near = lax.rem(geo, 2) == 1
    far = jnp.logical_not(near)

    def at_inner(d):
        return {"mem": outer * q + lax.rem(inner + d, q)}

    def at_outer(d):
        return {"mem": lax.rem(outer + d, o) * q + inner}

    barrier = pltpu.get_barrier_semaphore()
    targets = ([at_inner(d) for d in range(1, q)] + [at_outer(d) for d in range(1, o)]
               + [{"geo": lax.rem(geo + d, ng)} for d in range(1, ng)])
    for target in targets:
        pl.semaphore_signal(barrier, inc=1, device_id=target, device_id_type=pl.DeviceIdType.MESH)

    def landed(ref, sem):
        pltpu.make_async_copy(ref, ref, sem).wait()

    pert_cps = [pltpu.make_async_copy(pert_hbm.at[:, 0, :, pl.ds(c * cw, cw)], pert.at[:, :, pl.ds(c * cw, cw)], pert_sem.at[c])
                for c in range(nc)]
    for cp in pert_cps:
        cp.start()
    kidx_cp = pltpu.make_async_copy(kidx_hbm, kidx, loc_sem.at[1])
    kidx_cp.start()
    table_cp = pltpu.make_async_copy(table_hbm, table, loc_sem.at[2])
    table_cp.start()
    for l in range(lev):
        pltpu.make_async_copy(ctrl.at[0, l], C.at[:, l], loc_sem.at[3]).start()
    bands_cp = pltpu.make_async_copy(bands_hbm, bands, loc_sem.at[4])
    bands_cp.start()
    bounds_cp = pltpu.make_async_copy(bounds_hbm, bounds, loc_sem.at[5])
    bounds_cp.start()

    left = lax.broadcasted_iota(jnp.int32, (hy, hy), 0)
    right = lax.broadcasted_iota(jnp.int32, (hy, hy), 1)
    spread[...] = jnp.where(left == (right % LANES) * parts + right // LANES, 1.0, 0.0).astype(BF16)
    gather[...] = jnp.where(right == (left % LANES) * parts + left // LANES, 1.0, 0.0).astype(BF16)

    def piece(vals, i):
        return jnp.concatenate([v[(k * q + i) * lm:(k * q + i + 1) * lm] for v in vals for k in range(o)], axis=0)

    def strip(k):
        return pl.ds(pl.multiple_of(k * hy, LANES), hy)

    def repack(c):
        def step(r, carry):
            at = strip(c * cr + r)
            vals = [pert[v, :, at].astype(F32) for v in range(nvar)]
            for i in range(q):
                PS[i, c, :, strip(r)] = piece(vals, i).astype(BF16)
            return carry

        lax.fori_loop(0, cr, step, 0)

    def inner_send(src, dst, c, send, recv):
        for d in range(1, q):
            pltpu.make_async_remote_copy(
                src_ref=src.at[lax.rem(inner + d, q), c], dst_ref=dst.at[d, c], send_sem=send, recv_sem=recv,
                device_id=at_inner(d), device_id_type=pl.DeviceIdType.MESH).start()

    def offer(c, send):
        repack(c)
        inner_send(PS, PR, c, send, pr_sem.at[c])

    pl.semaphore_wait(barrier, len(targets))
    for c in range(nc):
        pert_cps[c].wait()
        if c < npc:
            pl.when(far)(functools.partial(offer, c, send_sem.at[5]))
        else:
            offer(c, send_sem.at[0])

    def turned(i, last):
        return jnp.where(backward, last - i, i)

    kidx_cp.wait()
    table_cp.wait()
    landed(C, loc_sem.at[3])
    x = C[...].reshape(hx * lev, hy)
    high = x.astype(BF16)
    low = (x - high.astype(F32)).astype(BF16)
    x = jnp.concatenate([kidx[...].astype(F32).astype(BF16), high, low], axis=0)
    x = jnp.dot(x, spread[...], preferred_element_type=F32)
    index = x[:hx]
    x = (x[hx:hx + hx * lev] + x[hx + hx * lev:]).reshape(hx, lev, hy)
    for i in range(hx):
        S[turned(i, hx - 1)] = x[i]
    field = jnp.zeros(index.shape, F32)
    for entry in range(table.shape[0]):
        field = jnp.where(index == float(entry), table[entry], field)
    kf[0:hx] = field
    kf[hx:] = jnp.zeros((kf.shape[0] - hx, hy), F32)
    east = 0.5 * (field + kf[1:hx + 1])
    lane = lax.broadcasted_iota(jnp.int32, (hx, LANES), 1)
    cut = [field[:, p * LANES:(p + 1) * LANES] for p in range(parts)]
    norths = [0.5 * (cut[p] + cut[p + 1]) for p in range(parts - 1)]
    last = 0.5 * (cut[-1] + pltpu.roll(cut[0], LANES - 1, axis=1))
    norths.append(jnp.where(lane < LANES - 1, last, 0.0))
    south = pltpu.roll(norths[-1], 1, axis=1)
    for i in range(hx):
        if i < hx - 1:
            WE[turned(i, hx - 2)] = jnp.broadcast_to(east[i:i + 1], (lev, hy))
        to = turned(i, hx - 1)
        for p in range(parts):
            WN[to, :, p * LANES:(p + 1) * LANES] = jnp.broadcast_to(norths[p][i:i + 1], (lev, LANES))
        WS[to] = jnp.broadcast_to(south[i:i + 1], (lev, LANES))

    def row_of(ref, i):
        return [ref[i, :, p * LANES:(p + 1) * LANES] for p in range(parts)]

    def sweep(it, lo, hi):
        s = row_of(S, lo)
        before = row_of(FL, it) if lo else None
        for i in range(lo, hi):
            wn = row_of(WN, i)
            ahead = s[1:] + [pltpu.roll(s[0], LANES - 1, axis=1)]
            flux = [wn[p] * (ahead[p] - s[p]) for p in range(parts)]
            behind = [WS[i] * (s[0] - pltpu.roll(s[-1], 1, axis=1))] + flux[:-1]
            new = [s[p] + (flux[p] - behind[p]) for p in range(parts)]
            if before is not None:
                new = [new[p] - before[p] for p in range(parts)]
            if i < hx - 1:
                after = row_of(S, i + 1)
                we = row_of(WE, i)
                before = [we[p] * (after[p] - s[p]) for p in range(parts)]
                new = [new[p] + before[p] for p in range(parts)]
                s = after
            for p in range(parts):
                S[i, :, p * LANES:(p + 1) * LANES] = new[p]
        if hi < hx:
            for p in range(parts):
                FL[it, :, p * LANES:(p + 1) * LANES] = before[p]

    half = ng // 2
    span = half * rows
    for b in range(2):
        for it in range(ITERS):
            lo, hi = (0, min(hx, span + ITERS - 1 - it)) if b == 0 else (min(hx, span + ITERS - 1 - it), hx)
            if hi > lo:
                sweep(it, lo, hi)
        if (span * lev) % 8 == 0:
            x = S[b * span:(b + 1) * span].reshape(span * lev, hy).astype(BF16)
            x = jnp.dot(x, gather[...], preferred_element_type=F32).reshape(span, lev, hy).astype(BF16)
        else:
            x = [jnp.dot(S[b * span + r].astype(BF16), gather[...], preferred_element_type=F32).astype(BF16)
                 for r in range(span)]
        for r in range(span):
            B[turned(b * span + r, hx - 1)] = x[r]
        for j in range(half):
            band = j + jnp.where(backward, half, 0) if b == 0 else j + jnp.where(backward, 0, half)
            cps = [pltpu.make_async_remote_copy(
                src_ref=B.at[pl.ds(band * rows + c * cr, cr)], dst_ref=G.at[geo, pl.ds(c * cr, cr)],
                send_sem=send_sem.at[1], recv_sem=gr_sem.at[c],
                device_id={"geo": band}, device_id_type=pl.DeviceIdType.MESH) for c in range(nc)]
            if b == 0:
                for cp in cps:
                    cp.start()
            else:
                @pl.when(band != geo)
                def _(cps=cps):
                    for cp in cps:
                        cp.start()

    for c in range(nc):
        pltpu.make_async_copy(B.at[pl.ds(geo * rows + c * cr, cr)], G.at[geo, pl.ds(c * cr, cr)], gr_sem.at[c]).start()

    bands_cp.wait()
    bounds_cp.wait()
    eye = (lax.broadcasted_iota(jnp.int32, (levels, levels), 0)
           == lax.broadcasted_iota(jnp.int32, (levels, levels), 1))
    for t in range(tiles):
        for k in range(nband):
            row = jnp.broadcast_to(bands[k, t:t + 1, :], (levels, levels))
            column = jnp.sum(jnp.where(eye, row, 0.0), axis=1, keepdims=True)
            bandsb[t, k] = jnp.broadcast_to(column, (levels, LANES))

    def coefficients(k, carry):
        at = pl.ds(pl.multiple_of(k * LANES, LANES), LANES)
        column = geo * cols + k * LANES + lax.broadcasted_iota(jnp.int32, (levels, LANES), 1)
        past = [column >= bounds[t] for t in range(1, tiles)]
        for k in range(nband):
            value = bandsb[0, k]
            for t in range(1, tiles):
                value = jnp.where(past[t - 1], bandsb[t, k], value)
            coef[k, :, at] = value
        return carry

    lax.fori_loop(0, cols // LANES, coefficients, 0)
    base = 8
    D[0:base, :] = jnp.zeros((base, cols), F32)
    D[base + levels:, :] = jnp.zeros((D.shape[0] - base - levels, cols), F32)

    def filtered(k):
        at = strip(k)
        value = D[base:base + levels, at]
        for n in range(nband):
            value = value + coef[n, :, at] * D[base + n - pad:base + n - pad + levels, at]
        return value.astype(BF16).astype(F32), at

    def vertical(c, products, send):
        def step(r, carry):
            k = c * cr + r
            for g in range(ng):
                D[base + g * lev:base + (g + 1) * lev, strip(k)] = G[g, k].astype(F32)
            value, at = filtered(k)
            if products:
                vals = [pert[v, :, at].astype(F32) * value for v in range(nvar)]
                for i in range(q):
                    XS[i, c, :, strip(r)] = piece(vals, i).astype(BF16)
            else:
                for i in range(q):
                    FS[i, c, :, strip(r)] = piece([value], i).astype(BF16)
            return carry

        lax.fori_loop(0, cr, step, 0)
        if products:
            inner_send(XS, XR, c, send, ar_sem.at[c])
        else:
            inner_send(FS, FR, c, send, ar_sem.at[c])

    for c in range(nc):
        landed(G.at[:, pl.ds(c * cr, cr)], gr_sem.at[c])
        if c < npc:
            pl.when(near)(functools.partial(vertical, c, True, send_sem.at[2]))
            pl.when(far)(functools.partial(vertical, c, False, send_sem.at[6]))
        else:
            vertical(c, False, send_sem.at[3])

    others = pl.ds(1, q - 1)

    def total(c, products):
        if products:
            landed(XR.at[others, c], ar_sem.at[c])
        else:
            landed(FR.at[others, c], ar_sem.at[c])
            landed(PR.at[others, c], pr_sem.at[c])

        def step(r, carry):
            at = strip(r)
            if products:
                acc = XS[inner, c, :, at].astype(F32)
                for d in range(1, q):
                    acc = acc + XR[d, c, :, at].astype(F32)
            else:
                f = FS[inner, c, :, at].astype(F32)
                acc = PS[inner, c, :, at].astype(F32) * jnp.concatenate([f] * nvar, axis=0)
                for d in range(1, q):
                    f = FR[d, c, :, at].astype(F32)
                    acc = acc + PR[d, c, :, at].astype(F32) * jnp.concatenate([f] * nvar, axis=0)
            shares = [jnp.concatenate([acc[v * wide + k * lm:v * wide + (k + 1) * lm] for v in range(nvar)], axis=0)
                      for k in range(o)]
            mine = shares[0]
            for k in range(o):
                YS[k, c, :, at] = shares[k].astype(BF16)
                if k:
                    mine = jnp.where(outer == k, shares[k], mine)
            OWN[c, :, at] = mine
            return carry

        lax.fori_loop(0, cr, step, 0)

    for c in range(nc):
        if c < npc:
            pl.when(near)(functools.partial(total, c, True))
            pl.when(far)(functools.partial(total, c, False))
        else:
            total(c, False)
        for d in range(1, o):
            pltpu.make_async_remote_copy(
                src_ref=YS.at[lax.rem(outer + d, o), c], dst_ref=YR.at[d, c], send_sem=send_sem.at[4], recv_sem=br_sem.at[c],
                device_id=at_outer(d), device_id_type=pl.DeviceIdType.MESH).start()

    for c in range(nc):
        landed(YR.at[pl.ds(1, o - 1), c], br_sem.at[c])

        def finish(r, carry, c=c):
            at = strip(r)
            acc = OWN[c, :, at]
            for d in range(1, o):
                acc = acc + YR[d, c, :, at].astype(F32)
            for v in range(nvar):
                out[v, :, strip(c * cr + r)] = acc[v * lm:(v + 1) * lm]
            return carry

        lax.fori_loop(0, cr, finish, 0)

    peers = pl.ds(0, q - 1)
    landed(PS.at[peers, pl.ds(npc, nc - npc)], send_sem.at[0])
    landed(B.at[pl.ds(0, hx - rows)], send_sem.at[1])
    landed(FS.at[peers, pl.ds(npc, nc - npc)], send_sem.at[3])
    landed(YS.at[pl.ds(0, o - 1)], send_sem.at[4])

    @pl.when(near)
    def _():
        landed(XS.at[peers], send_sem.at[2])

    @pl.when(far)
    def _():
        landed(PS.at[peers, pl.ds(0, npc)], send_sem.at[5])
        landed(FS.at[peers, pl.ds(0, npc)], send_sem.at[6])


def body(nm, ng, control, kappa_table, kappa_index, tile_bounds, filter_bands, perturbation):
    _, lev, hx, hy = control.shape
    nvar, _, levels, cols = perturbation.shape
    lm = levels // nm
    rows = hx // ng
    tiles, nband, _ = filter_bands.shape
    q = inner_size(nm)
    o = nm // q
    wide = levels // q
    cr = max(1, rows // 6)
    nc = rows // cr
    npc = nc // 2
    cw = cr * hy
    dma = pltpu.SemaphoreType.DMA
    hbm = pl.BlockSpec(memory_space=pl.ANY)
    return pl.pallas_call(
        functools.partial(kernel, nm, ng, q),
        out_shape=pltpu.VMEM((nvar, lm, cols), F32),
        in_specs=[hbm] * 6,
        out_specs=pl.BlockSpec(memory_space=pltpu.VMEM),
        scratch_shapes=[
            pltpu.SMEM(kappa_table.shape, F32),
            pltpu.SMEM(tile_bounds.shape, jnp.int32),
            pltpu.VMEM((hx, lev, hy), F32),
            pltpu.VMEM((hx, lev, hy), F32),
            pltpu.VMEM((hx, lev, hy), F32),
            pltpu.VMEM((hx, lev, hy), F32),
            pltpu.VMEM((hx, lev, LANES), F32),
            pltpu.VMEM((ITERS, lev, hy), F32),
            pltpu.VMEM((hy, hy), BF16),
            pltpu.VMEM((hy, hy), BF16),
            pltpu.VMEM((hx, hy), jnp.int32),
            pltpu.VMEM((hx + 8, hy), F32),
            pltpu.VMEM((nband, tiles, levels), F32),
            pltpu.VMEM((tiles, nband, levels, LANES), F32),
            pltpu.VMEM((nband, levels, cols), F32),
            pltpu.VMEM((nvar, levels, cols), BF16),
            pltpu.VMEM((q, nc, nvar * wide, cw), BF16),
            pltpu.VMEM((q, nc, nvar * wide, cw), BF16),
            pltpu.VMEM((hx, lev, hy), BF16),
            pltpu.VMEM((ng, rows, lev, hy), BF16),
            pltpu.VMEM((levels + 16, cols), F32),
            pltpu.VMEM((q, nc, wide, cw), BF16),
            pltpu.VMEM((q, nc, wide, cw), BF16),
            pltpu.VMEM((q, npc, nvar * wide, cw), BF16),
            pltpu.VMEM((q, npc, nvar * wide, cw), BF16),
            pltpu.VMEM((nc, nvar * lm, cw), F32),
            pltpu.VMEM((o, nc, nvar * lm, cw), BF16),
            pltpu.VMEM((o, nc, nvar * lm, cw), BF16),
            dma((6,)), dma((nc,)), dma((7,)), dma((nc,)), dma((nc,)), dma((nc,)), dma((nc,)),
        ],
        compiler_params=pltpu.CompilerParams(
            collective_id=0, has_side_effects=True, vmem_limit_bytes=56 * 2**20),
    )(control, kappa_table, kappa_index, tile_bounds, jnp.swapaxes(filter_bands, 0, 1), perturbation)


def solution(mesh):
    in_specs = (P("mem", "geo", None, None), P(), P(), P(), P(), P(None, "mem", None, "geo"))
    out_specs = P(None, "mem", "geo")
    run = functools.partial(body, mesh.shape["mem"], mesh.shape["geo"])
    return jax.shard_map(run, mesh=mesh, in_specs=in_specs, out_specs=out_specs, check_vma=False)
```

```python
import functools

import jax
import jax.numpy as jnp
from jax import lax
from jax.experimental import pallas as pl
from jax.experimental.pallas import tpu as pltpu
from jax.sharding import PartitionSpec as P

ITERS = 10
F32, BF16 = jnp.float32, jnp.bfloat16
LANES = 128


def inner_size(nm):
    q = 1
    while nm % (2 * q) == 0 and (2 * q) ** 2 <= 2 * nm:
        q *= 2
    return q


def kernel(nm, ng, q, ctrl, table_hbm, kidx_hbm, bounds_hbm, bands_hbm, pert_hbm, out,
           table, bounds, C, S, WE, WN, WS, FL, spread, gather, kidx, kf, bands, bandsb, coef, pert,
           PS, PR, B, G, D, FS, FR, XS, XR, YS, YR,
           loc_sem, pert_sem, send_sem, pr_sem, gr_sem, ar_sem, zr_sem, br_sem):
    mem = lax.axis_index("mem")
    geo = lax.axis_index("geo")
    o = nm // q
    inner = lax.rem(mem, q)
    outer = mem // q
    hx, lev, hy = S.shape
    nvar, levels, cols = pert.shape
    lm = levels // nm
    rows = hx // ng
    nband, tiles, _ = bands.shape
    parts = hy // LANES
    pad = nband // 2
    nc = YS.shape[1]
    cr = rows // nc
    cw = cr * hy
    npc = XS.shape[1]
    backward = geo < ng // 2
    near = lax.rem(geo, 2) == 1
    far = jnp.logical_not(near)

    def at_inner(d):
        return {"mem": outer * q + lax.rem(inner + d, q)}

    def at_outer(d):
        return {"mem": lax.rem(outer + d, o) * q + inner}

    barrier = pltpu.get_barrier_semaphore()
    targets = ([at_inner(d) for d in range(1, q)] + [at_outer(d) for d in range(1, o)]
               + [{"geo": lax.rem(geo + d, ng)} for d in range(1, ng)])
    for target in targets:
        pl.semaphore_signal(barrier, inc=1, device_id=target, device_id_type=pl.DeviceIdType.MESH)

    def landed(ref, sem):
        pltpu.make_async_copy(ref, ref, sem).wait()

    pert_cps = [pltpu.make_async_copy(pert_hbm.at[:, 0, :, pl.ds(c * cw, cw)], pert.at[:, :, pl.ds(c * cw, cw)], pert_sem.at[c])
                for c in range(nc)]
    for cp in pert_cps:
        cp.start()
    kidx_cp = pltpu.make_async_copy(kidx_hbm, kidx, loc_sem.at[0])
    kidx_cp.start()
    table_cp = pltpu.make_async_copy(table_hbm, table, loc_sem.at[1])
    table_cp.start()
    for l in range(lev):
        pltpu.make_async_copy(ctrl.at[0, l], C.at[:, l], loc_sem.at[2]).start()
    left = lax.broadcasted_iota(jnp.int32, (hy, hy), 0)
    right = lax.broadcasted_iota(jnp.int32, (hy, hy), 1)
    spread[...] = jnp.where(left == (right % LANES) * parts + right // LANES, 1.0, 0.0).astype(BF16)
    gather[...] = jnp.where(right == (left % LANES) * parts + left // LANES, 1.0, 0.0).astype(BF16)

    def piece(vals, i, k):
        return jnp.concatenate([v[(k * q + i) * lm:(k * q + i + 1) * lm] for v in vals], axis=0)

    def split(ref, vals, c, at):
        for k in range(o):
            slot = lax.rem(k - outer + o, o)
            for i in range(q):
                ref[i, c, slot, :, at] = piece(vals, i, k).astype(BF16)

    def strip(k):
        return pl.ds(pl.multiple_of(k * hy, LANES), hy)

    def repack(c):
        def step(r, carry):
            at = strip(c * cr + r)
            vals = [pert[v, :, at].astype(F32) for v in range(nvar)]
            split(PS, vals, c, strip(r))
            return carry

        lax.fori_loop(0, cr, step, 0)

    crossing = pl.ds(1, o - 1)
    whole = pl.ds(0, o)
    staying = pl.ds(0, 1)

    def inner_send(src, dst, c, part, send, recv):
        for d in range(1, q):
            pltpu.make_async_remote_copy(
                src_ref=src.at[lax.rem(inner + d, q), c, part], dst_ref=dst.at[d, c, part], send_sem=send, recv_sem=recv,
                device_id=at_inner(d), device_id_type=pl.DeviceIdType.MESH).start()

    def offer(c):
        repack(c)
        inner_send(PS, PR, c, whole, send_sem.at[0], pr_sem.at[0 if c >= npc else 1])

    pl.semaphore_wait(barrier, len(targets))
    for c in range(nc):
        pert_cps[c].wait()
        if c < npc:
            pl.when(far)(functools.partial(offer, c))
        else:
            offer(c)

    def turned(i, last):
        return jnp.where(backward, last - i, i)

    kidx_cp.wait()
    table_cp.wait()
    landed(C, loc_sem.at[2])
    x = C[...].reshape(hx * lev, hy)
    high = x.astype(BF16)
    low = (x - high.astype(F32)).astype(BF16)
    x = jnp.concatenate([kidx[...].astype(F32).astype(BF16), high, low], axis=0)
    x = jnp.dot(x, spread[...], preferred_element_type=F32)
    index = x[:hx]
    x = (x[hx:hx + hx * lev] + x[hx + hx * lev:]).reshape(hx, lev, hy)
    for i in range(hx):
        S[turned(i, hx - 1)] = x[i]
    field = jnp.zeros(index.shape, F32)
    for entry in range(table.shape[0]):
        field = jnp.where(index == float(entry), table[entry], field)
    kf[0:hx] = field
    kf[hx:] = jnp.zeros((kf.shape[0] - hx, hy), F32)
    east = 0.5 * (field + kf[1:hx + 1])
    lane = lax.broadcasted_iota(jnp.int32, (hx, LANES), 1)
    cut = [field[:, p * LANES:(p + 1) * LANES] for p in range(parts)]
    norths = [0.5 * (cut[p] + cut[p + 1]) for p in range(parts - 1)]
    last = 0.5 * (cut[-1] + pltpu.roll(cut[0], LANES - 1, axis=1))
    norths.append(jnp.where(lane < LANES - 1, last, 0.0))
    south = pltpu.roll(norths[-1], 1, axis=1)
    for i in range(hx):
        if i < hx - 1:
            WE[turned(i, hx - 2)] = jnp.broadcast_to(east[i:i + 1], (lev, hy))
        to = turned(i, hx - 1)
        for p in range(parts):
            WN[to, :, p * LANES:(p + 1) * LANES] = jnp.broadcast_to(norths[p][i:i + 1], (lev, LANES))
        WS[to] = jnp.broadcast_to(south[i:i + 1], (lev, LANES))

    bands_cp = pltpu.make_async_copy(bands_hbm, bands, loc_sem.at[0])
    bands_cp.start()
    bounds_cp = pltpu.make_async_copy(bounds_hbm, bounds, loc_sem.at[1])
    bounds_cp.start()

    def row_of(ref, i):
        return [ref[i, :, p * LANES:(p + 1) * LANES] for p in range(parts)]

    def sweep(it, lo, hi):
        s = row_of(S, lo)
        before = row_of(FL, it) if lo else None
        for i in range(lo, hi):
            wn = row_of(WN, i)
            ahead = s[1:] + [pltpu.roll(s[0], LANES - 1, axis=1)]
            flux = [wn[p] * (ahead[p] - s[p]) for p in range(parts)]
            behind = [WS[i] * (s[0] - pltpu.roll(s[-1], 1, axis=1))] + flux[:-1]
            new = [s[p] + (flux[p] - behind[p]) for p in range(parts)]
            if before is not None:
                new = [new[p] - before[p] for p in range(parts)]
            if i < hx - 1:
                after = row_of(S, i + 1)
                we = row_of(WE, i)
                before = [we[p] * (after[p] - s[p]) for p in range(parts)]
                new = [new[p] + before[p] for p in range(parts)]
                s = after
            for p in range(parts):
                S[i, :, p * LANES:(p + 1) * LANES] = new[p]
        if hi < hx:
            for p in range(parts):
                FL[it, :, p * LANES:(p + 1) * LANES] = before[p]

    half = ng // 2
    span = half * rows
    for b in range(2):
        for it in range(ITERS):
            lo, hi = (0, min(hx, span + ITERS - 1 - it)) if b == 0 else (min(hx, span + ITERS - 1 - it), hx)
            if hi > lo:
                sweep(it, lo, hi)
        if (span * lev) % 8 == 0:
            x = S[b * span:(b + 1) * span].reshape(span * lev, hy).astype(BF16)
            x = jnp.dot(x, gather[...], preferred_element_type=F32).reshape(span, lev, hy).astype(BF16)
        else:
            x = [jnp.dot(S[b * span + r].astype(BF16), gather[...], preferred_element_type=F32).astype(BF16)
                 for r in range(span)]
        for r in range(span):
            B[turned(b * span + r, hx - 1)] = x[r]
        for j in range(half):
            band = j + jnp.where(backward, half, 0) if b == 0 else j + jnp.where(backward, 0, half)
            cps = [pltpu.make_async_remote_copy(
                src_ref=B.at[pl.ds(band * rows + c * cr, cr)], dst_ref=G.at[geo, pl.ds(c * cr, cr)],
                send_sem=send_sem.at[1], recv_sem=gr_sem.at[c],
                device_id={"geo": band}, device_id_type=pl.DeviceIdType.MESH) for c in range(nc)]
            if b == 0:
                for cp in cps:
                    cp.start()
            else:
                @pl.when(band != geo)
                def _(cps=cps):
                    for cp in cps:
                        cp.start()

    for c in range(nc):
        pltpu.make_async_copy(B.at[pl.ds(geo * rows + c * cr, cr)], G.at[geo, pl.ds(c * cr, cr)], gr_sem.at[c]).start()

    bands_cp.wait()
    bounds_cp.wait()
    eye = (lax.broadcasted_iota(jnp.int32, (levels, levels), 0)
           == lax.broadcasted_iota(jnp.int32, (levels, levels), 1))
    for t in range(tiles):
        for k in range(nband):
            row = jnp.broadcast_to(bands[k, t:t + 1, :], (levels, levels))
            column = jnp.sum(jnp.where(eye, row, 0.0), axis=1, keepdims=True)
            bandsb[t, k] = jnp.broadcast_to(column, (levels, LANES))

    def coefficients(k, carry):
        at = pl.ds(pl.multiple_of(k * LANES, LANES), LANES)
        column = geo * cols + k * LANES + lax.broadcasted_iota(jnp.int32, (levels, LANES), 1)
        past = [column >= bounds[t] for t in range(1, tiles)]
        for k in range(nband):
            value = bandsb[0, k]
            for t in range(1, tiles):
                value = jnp.where(past[t - 1], bandsb[t, k], value)
            coef[k, :, at] = value
        return carry

    lax.fori_loop(0, cols // LANES, coefficients, 0)
    base = 8
    D[0:base, :] = jnp.zeros((base, cols), F32)
    D[base + levels:, :] = jnp.zeros((D.shape[0] - base - levels, cols), F32)

    def filtered(k):
        at = strip(k)
        value = D[base:base + levels, at]
        for n in range(nband):
            value = value + coef[n, :, at] * D[base + n - pad:base + n - pad + levels, at]
        return value.astype(BF16).astype(F32), at

    def vertical(c, products):
        def step(r, carry):
            k = c * cr + r
            for g in range(ng):
                D[base + g * lev:base + (g + 1) * lev, strip(k)] = G[g, k].astype(F32)
            value, at = filtered(k)
            if products:
                vals = [pert[v, :, at].astype(F32) * value for v in range(nvar)]
                split(XS, vals, c, strip(r))
            else:
                split(FS, [value], c, strip(r))
            return carry

        lax.fori_loop(0, cr, step, 0)

    def hand(c, products, part, send, recv):
        if products:
            inner_send(XS, XR, c, part, send, recv.at[c])
        else:
            inner_send(FS, FR, c, part, send, recv.at[c])

    def vertical_send(c, products, send):
        vertical(c, products)
        hand(c, products, crossing, send, ar_sem)

    for c in range(nc):
        landed(G.at[:, pl.ds(c * cr, cr)], gr_sem.at[c])
        if c < npc:
            pl.when(near)(functools.partial(vertical_send, c, True, send_sem.at[2]))
            pl.when(far)(functools.partial(vertical_send, c, False, send_sem.at[3]))
        else:
            vertical_send(c, False, send_sem.at[3])

    def later(c):
        if c < npc:
            pl.when(near)(functools.partial(hand, c, True, staying, send_sem.at[2], zr_sem))
            pl.when(far)(functools.partial(hand, c, False, staying, send_sem.at[3], zr_sem))
        else:
            hand(c, False, staying, send_sem.at[3], zr_sem)

    others = pl.ds(1, q - 1)

    def summed(c, k, at, products):
        if products:
            acc = XS[inner, c, k, :, at].astype(F32)
            for d in range(1, q):
                acc = acc + XR[d, c, k, :, at].astype(F32)
        else:
            f = FS[inner, c, k, :, at].astype(F32)
            acc = PS[inner, c, k, :, at].astype(F32) * jnp.concatenate([f] * nvar, axis=0)
            for d in range(1, q):
                f = FR[d, c, k, :, at].astype(F32)
                acc = acc + PR[d, c, k, :, at].astype(F32) * jnp.concatenate([f] * nvar, axis=0)
        return acc

    def cross(c, products):
        landed((XR if products else FR).at[others, c, crossing], ar_sem.at[c])
        if not products and c == 0:
            landed(PR.at[others, pl.ds(0, npc)], pr_sem.at[1])
        if c == npc:
            landed(PR.at[others, pl.ds(npc, nc - npc)], pr_sem.at[0])

        def step(r, carry):
            at = strip(r)
            for k in range(1, o):
                YS[k, c, :, at] = summed(c, k, at, products).astype(BF16)
            return carry

        lax.fori_loop(0, cr, step, 0)
        for k in range(1, o):
            pltpu.make_async_remote_copy(
                src_ref=YS.at[k, c], dst_ref=YR.at[k, c], send_sem=send_sem.at[4], recv_sem=br_sem.at[c],
                device_id=at_outer(k), device_id_type=pl.DeviceIdType.MESH).start()

    def finish(c, products):
        landed((XR if products else FR).at[others, c, staying], zr_sem.at[c])
        landed(YR.at[crossing, c], br_sem.at[c])

        def step(r, carry):
            at = strip(r)
            acc = summed(c, 0, at, products)
            for k in range(1, o):
                acc = acc + YR[k, c, :, at].astype(F32)
            for v in range(nvar):
                out[v, :, strip(c * cr + r)] = acc[v * lm:(v + 1) * lm]
            return carry

        lax.fori_loop(0, cr, step, 0)

    def each(act, c):
        if c < npc:
            pl.when(near)(functools.partial(act, c, True))
            pl.when(far)(functools.partial(act, c, False))
        else:
            act(c, False)

    each(cross, 0)
    for c in range(nc):
        later(c)
    for c in range(1, nc):
        each(cross, c)
    for c in range(nc):
        each(finish, c)

    peers = pl.ds(0, q - 1)
    landed(B.at[pl.ds(0, hx - rows)], send_sem.at[1])
    landed(YS.at[crossing], send_sem.at[4])

    @pl.when(near)
    def _():
        landed(PS.at[peers, pl.ds(npc, nc - npc)], send_sem.at[0])
        landed(XS.at[peers], send_sem.at[2])
        landed(FS.at[peers, pl.ds(npc, nc - npc)], send_sem.at[3])

    @pl.when(far)
    def _():
        landed(PS.at[peers], send_sem.at[0])
        landed(FS.at[peers], send_sem.at[3])


def body(nm, ng, control, kappa_table, kappa_index, tile_bounds, filter_bands, perturbation):
    _, lev, hx, hy = control.shape
    nvar, _, levels, cols = perturbation.shape
    lm = levels // nm
    rows = hx // ng
    tiles, nband, _ = filter_bands.shape
    q = inner_size(nm)
    o = nm // q
    cr = max(1, rows // 6)
    nc = rows // cr
    npc = 1
    cw = cr * hy
    dma = pltpu.SemaphoreType.DMA
    hbm = pl.BlockSpec(memory_space=pl.ANY)
    return pl.pallas_call(
        functools.partial(kernel, nm, ng, q),
        out_shape=pltpu.VMEM((nvar, lm, cols), F32),
        in_specs=[hbm] * 6,
        out_specs=pl.BlockSpec(memory_space=pltpu.VMEM),
        scratch_shapes=[
            pltpu.SMEM(kappa_table.shape, F32),
            pltpu.SMEM(tile_bounds.shape, jnp.int32),
            pltpu.VMEM((hx, lev, hy), F32),
            pltpu.VMEM((hx, lev, hy), F32),
            pltpu.VMEM((hx, lev, hy), F32),
            pltpu.VMEM((hx, lev, hy), F32),
            pltpu.VMEM((hx, lev, LANES), F32),
            pltpu.VMEM((ITERS, lev, hy), F32),
            pltpu.VMEM((hy, hy), BF16),
            pltpu.VMEM((hy, hy), BF16),
            pltpu.VMEM((hx, hy), jnp.int32),
            pltpu.VMEM((hx + 8, hy), F32),
            pltpu.VMEM((nband, tiles, levels), F32),
            pltpu.VMEM((tiles, nband, levels, LANES), F32),
            pltpu.VMEM((nband, levels, cols), F32),
            pltpu.VMEM((nvar, levels, cols), BF16),
            pltpu.VMEM((q, nc, o, nvar * lm, cw), BF16),
            pltpu.VMEM((q, nc, o, nvar * lm, cw), BF16),
            pltpu.VMEM((hx, lev, hy), BF16),
            pltpu.VMEM((ng, rows, lev, hy), BF16),
            pltpu.VMEM((levels + 16, cols), F32),
            pltpu.VMEM((q, nc, o, lm, cw), BF16),
            pltpu.VMEM((q, nc, o, lm, cw), BF16),
            pltpu.VMEM((q, npc, o, nvar * lm, cw), BF16),
            pltpu.VMEM((q, npc, o, nvar * lm, cw), BF16),
            pltpu.VMEM((o, nc, nvar * lm, cw), BF16),
            pltpu.VMEM((o, nc, nvar * lm, cw), BF16),
            dma((3,)), dma((nc,)), dma((5,)), dma((2,)), dma((nc,)), dma((nc,)), dma((nc,)), dma((nc,)),
        ],
        compiler_params=pltpu.CompilerParams(
            collective_id=0, has_side_effects=True, vmem_limit_bytes=56 * 2**20),
    )(control, kappa_table, kappa_index, tile_bounds, jnp.swapaxes(filter_bands, 0, 1), perturbation)


def solution(mesh):
    in_specs = (P("mem", "geo", None, None), P(), P(), P(), P(), P(None, "mem", None, "geo"))
    out_specs = P(None, "mem", "geo")
    run = functools.partial(body, mesh.shape["mem"], mesh.shape["geo"])
    return jax.shard_map(run, mesh=mesh, in_specs=in_specs, out_specs=out_specs, check_vma=False)
```

```python
import functools

import jax
import jax.numpy as jnp
from jax import lax
from jax.experimental import pallas as pl
from jax.experimental.pallas import tpu as pltpu
from jax.sharding import PartitionSpec as P

ITERS = 10
F32, BF16 = jnp.float32, jnp.bfloat16
LANES = 128


def inner_size(nm):
    q = 1
    while nm % (2 * q) == 0 and (2 * q) ** 2 <= 2 * nm:
        q *= 2
    return q


def kernel(nm, ng, q, ctrl, table_hbm, kidx_hbm, bounds_hbm, bands_hbm, pert_hbm, out,
           table, bounds, C, S, WE, WN, WS, FL, spread, gather, kidx, kf, bands, bandsb, coef, pert,
           PS, PR, B, G, D, FS, FR, XS, XR, YS, YR,
           loc_sem, pert_sem, send_sem, pr_sem, gr_sem, ar_sem, zr_sem, br_sem):
    mem = lax.axis_index("mem")
    geo = lax.axis_index("geo")
    o = nm // q
    inner = lax.rem(mem, q)
    outer = mem // q
    hx, lev, hy = S.shape
    nvar, levels, cols = pert.shape
    lm = levels // nm
    rows = hx // ng
    nband, tiles, _ = bands.shape
    parts = hy // LANES
    pad = nband // 2
    nc = YS.shape[1]
    cr = rows // nc
    cw = cr * hy
    npc = XS.shape[1]
    backward = geo < ng // 2
    near = lax.rem(geo, 2) == 1
    far = jnp.logical_not(near)

    def at_inner(d):
        return {"mem": outer * q + lax.rem(inner + d, q)}

    def at_outer(d):
        return {"mem": lax.rem(outer + d, o) * q + inner}

    barrier = pltpu.get_barrier_semaphore()
    targets = ([at_inner(d) for d in range(1, q)] + [at_outer(d) for d in range(1, o)]
               + [{"geo": lax.rem(geo + d, ng)} for d in range(1, ng)])
    for target in targets:
        pl.semaphore_signal(barrier, inc=1, device_id=target, device_id_type=pl.DeviceIdType.MESH)

    def landed(ref, sem):
        pltpu.make_async_copy(ref, ref, sem).wait()

    pert_cps = [pltpu.make_async_copy(pert_hbm.at[:, 0, :, pl.ds(c * cw, cw)], pert.at[:, :, pl.ds(c * cw, cw)], pert_sem.at[c])
                for c in range(nc)]
    for cp in pert_cps:
        cp.start()
    kidx_cp = pltpu.make_async_copy(kidx_hbm, kidx, loc_sem.at[0])
    kidx_cp.start()
    table_cp = pltpu.make_async_copy(table_hbm, table, loc_sem.at[1])
    table_cp.start()
    for l in range(lev):
        pltpu.make_async_copy(ctrl.at[0, l], C.at[:, l], loc_sem.at[2]).start()
    left = lax.broadcasted_iota(jnp.int32, (hy, hy), 0)
    right = lax.broadcasted_iota(jnp.int32, (hy, hy), 1)
    spread[...] = jnp.where(left == (right % LANES) * parts + right // LANES, 1.0, 0.0).astype(BF16)
    gather[...] = jnp.where(right == (left % LANES) * parts + left // LANES, 1.0, 0.0).astype(BF16)

    def piece(vals, i, k):
        return jnp.concatenate([v[(k * q + i) * lm:(k * q + i + 1) * lm] for v in vals], axis=0)

    def split(ref, vals, c, at):
        for k in range(o):
            slot = lax.rem(k - outer + o, o)
            for i in range(q):
                ref[i, c, slot, :, at] = piece(vals, i, k).astype(BF16)

    def strip(k):
        return pl.ds(pl.multiple_of(k * hy, LANES), hy)

    def repack(c):
        def step(r, carry):
            at = strip(c * cr + r)
            vals = [pert[v, :, at].astype(F32) for v in range(nvar)]
            split(PS, vals, c, strip(r))
            return carry

        lax.fori_loop(0, cr, step, 0)

    crossing = pl.ds(1, o - 1)
    whole = pl.ds(0, o)
    staying = pl.ds(0, 1)

    def inner_send(src, dst, c, part, send, recv):
        for d in range(1, q):
            pltpu.make_async_remote_copy(
                src_ref=src.at[lax.rem(inner + d, q), c, part], dst_ref=dst.at[d, c, part], send_sem=send, recv_sem=recv,
                device_id=at_inner(d), device_id_type=pl.DeviceIdType.MESH).start()

    def offer(c):
        repack(c)
        inner_send(PS, PR, c, whole, send_sem.at[0], pr_sem.at[0 if c >= npc else 1])

    pl.semaphore_wait(barrier, len(targets))
    for c in range(nc):
        pert_cps[c].wait()
        if c < npc:
            pl.when(far)(functools.partial(offer, c))
        else:
            offer(c)

    def turned(i, last):
        return jnp.where(backward, last - i, i)

    kidx_cp.wait()
    table_cp.wait()
    landed(C, loc_sem.at[2])
    x = C[...].reshape(hx * lev, hy)
    high = x.astype(BF16)
    low = (x - high.astype(F32)).astype(BF16)
    x = jnp.concatenate([kidx[...].astype(F32).astype(BF16), high, low], axis=0)
    x = jnp.dot(x, spread[...], preferred_element_type=F32)
    index = x[:hx]
    x = (x[hx:hx + hx * lev] + x[hx + hx * lev:]).reshape(hx, lev, hy)
    for i in range(hx):
        S[turned(i, hx - 1)] = x[i]
    field = jnp.zeros(index.shape, F32)
    for entry in range(table.shape[0]):
        field = jnp.where(index == float(entry), table[entry], field)
    kf[0:hx] = field
    kf[hx:] = jnp.zeros((kf.shape[0] - hx, hy), F32)
    east = 0.5 * (field + kf[1:hx + 1])
    lane = lax.broadcasted_iota(jnp.int32, (hx, LANES), 1)
    cut = [field[:, p * LANES:(p + 1) * LANES] for p in range(parts)]
    norths = [0.5 * (cut[p] + cut[p + 1]) for p in range(parts - 1)]
    last = 0.5 * (cut[-1] + pltpu.roll(cut[0], LANES - 1, axis=1))
    norths.append(jnp.where(lane < LANES - 1, last, 0.0))
    south = pltpu.roll(norths[-1], 1, axis=1)
    for i in range(hx):
        if i < hx - 1:
            WE[turned(i, hx - 2)] = jnp.broadcast_to(east[i:i + 1], (lev, hy))
        to = turned(i, hx - 1)
        for p in range(parts):
            WN[to, :, p * LANES:(p + 1) * LANES] = jnp.broadcast_to(norths[p][i:i + 1], (lev, LANES))
        WS[to] = jnp.broadcast_to(south[i:i + 1], (lev, LANES))

    bands_cp = pltpu.make_async_copy(bands_hbm, bands, loc_sem.at[0])
    bands_cp.start()
    bounds_cp = pltpu.make_async_copy(bounds_hbm, bounds, loc_sem.at[1])
    bounds_cp.start()

    def row_of(ref, i):
        return [ref[i, :, p * LANES:(p + 1) * LANES] for p in range(parts)]

    def sweep(it, lo, hi):
        s = row_of(S, lo)
        before = row_of(FL, it) if lo else None
        for i in range(lo, hi):
            wn = row_of(WN, i)
            ahead = s[1:] + [pltpu.roll(s[0], LANES - 1, axis=1)]
            flux = [wn[p] * (ahead[p] - s[p]) for p in range(parts)]
            behind = [WS[i] * (s[0] - pltpu.roll(s[-1], 1, axis=1))] + flux[:-1]
            new = [s[p] + (flux[p] - behind[p]) for p in range(parts)]
            if before is not None:
                new = [new[p] - before[p] for p in range(parts)]
            if i < hx - 1:
                after = row_of(S, i + 1)
                we = row_of(WE, i)
                before = [we[p] * (after[p] - s[p]) for p in range(parts)]
                new = [new[p] + before[p] for p in range(parts)]
                s = after
            for p in range(parts):
                S[i, :, p * LANES:(p + 1) * LANES] = new[p]
        if hi < hx:
            for p in range(parts):
                FL[it, :, p * LANES:(p + 1) * LANES] = before[p]

    half = ng // 2
    span = half * rows
    for b in range(2):
        for it in range(ITERS):
            lo, hi = (0, min(hx, span + ITERS - 1 - it)) if b == 0 else (min(hx, span + ITERS - 1 - it), hx)
            if hi > lo:
                sweep(it, lo, hi)
        if (span * lev) % 8 == 0:
            x = S[b * span:(b + 1) * span].reshape(span * lev, hy).astype(BF16)
            x = jnp.dot(x, gather[...], preferred_element_type=F32).reshape(span, lev, hy).astype(BF16)
        else:
            x = [jnp.dot(S[b * span + r].astype(BF16), gather[...], preferred_element_type=F32).astype(BF16)
                 for r in range(span)]
        for r in range(span):
            B[turned(b * span + r, hx - 1)] = x[r]
        for j in range(half):
            band = j + jnp.where(backward, half, 0) if b == 0 else j + jnp.where(backward, 0, half)
            cps = [pltpu.make_async_remote_copy(
                src_ref=B.at[pl.ds(band * rows + c * cr, cr)], dst_ref=G.at[geo, pl.ds(c * cr, cr)],
                send_sem=send_sem.at[1], recv_sem=gr_sem.at[c],
                device_id={"geo": band}, device_id_type=pl.DeviceIdType.MESH) for c in range(nc)]
            if b == 0:
                for cp in cps:
                    cp.start()
            else:
                @pl.when(band != geo)
                def _(cps=cps):
                    for cp in cps:
                        cp.start()

    for c in range(nc):
        pltpu.make_async_copy(B.at[pl.ds(geo * rows + c * cr, cr)], G.at[geo, pl.ds(c * cr, cr)], gr_sem.at[c]).start()

    bands_cp.wait()
    bounds_cp.wait()
    eye = (lax.broadcasted_iota(jnp.int32, (levels, levels), 0)
           == lax.broadcasted_iota(jnp.int32, (levels, levels), 1))
    for t in range(tiles):
        for k in range(nband):
            row = jnp.broadcast_to(bands[k, t:t + 1, :], (levels, levels))
            column = jnp.sum(jnp.where(eye, row, 0.0), axis=1, keepdims=True)
            bandsb[t, k] = jnp.broadcast_to(column, (levels, LANES))

    def coefficients(k, carry):
        at = pl.ds(pl.multiple_of(k * LANES, LANES), LANES)
        column = geo * cols + k * LANES + lax.broadcasted_iota(jnp.int32, (levels, LANES), 1)
        past = [column >= bounds[t] for t in range(1, tiles)]
        for k in range(nband):
            value = bandsb[0, k]
            for t in range(1, tiles):
                value = jnp.where(past[t - 1], bandsb[t, k], value)
            coef[k, :, at] = value
        return carry

    lax.fori_loop(0, cols // LANES, coefficients, 0)
    base = 8
    D[0:base, :] = jnp.zeros((base, cols), F32)
    D[base + levels:, :] = jnp.zeros((D.shape[0] - base - levels, cols), F32)

    def filtered(k):
        at = strip(k)
        value = D[base:base + levels, at]
        for n in range(nband):
            value = value + coef[n, :, at] * D[base + n - pad:base + n - pad + levels, at]
        return value.astype(BF16).astype(F32), at

    def vertical(c, products):
        def step(r, carry):
            k = c * cr + r
            for g in range(ng):
                D[base + g * lev:base + (g + 1) * lev, strip(k)] = G[g, k].astype(F32)
            value, at = filtered(k)
            if products:
                vals = [pert[v, :, at].astype(F32) * value for v in range(nvar)]
                split(XS, vals, c, strip(r))
            else:
                split(FS, [value], c, strip(r))
            return carry

        lax.fori_loop(0, cr, step, 0)

    def hand(c, products, part, send, recv):
        if products:
            inner_send(XS, XR, c, part, send, recv.at[c])
        else:
            inner_send(FS, FR, c, part, send, recv.at[c])

    def vertical_send(c, products, send):
        vertical(c, products)
        hand(c, products, crossing, send, ar_sem)

    for c in range(nc):
        landed(G.at[:, pl.ds(c * cr, cr)], gr_sem.at[c])
        if c < npc:
            pl.when(near)(functools.partial(vertical_send, c, True, send_sem.at[2]))
            pl.when(far)(functools.partial(vertical_send, c, False, send_sem.at[3]))
        else:
            vertical_send(c, False, send_sem.at[3])

    def later(c):
        if c < npc:
            pl.when(near)(functools.partial(hand, c, True, staying, send_sem.at[2], zr_sem))
            pl.when(far)(functools.partial(hand, c, False, staying, send_sem.at[3], zr_sem))
        else:
            hand(c, False, staying, send_sem.at[3], zr_sem)

    others = pl.ds(1, q - 1)

    def summed(c, k, at, products):
        if products:
            acc = XS[inner, c, k, :, at].astype(F32)
            for d in range(1, q):
                acc = acc + XR[d, c, k, :, at].astype(F32)
        else:
            f = FS[inner, c, k, :, at].astype(F32)
            acc = PS[inner, c, k, :, at].astype(F32) * jnp.concatenate([f] * nvar, axis=0)
            for d in range(1, q):
                f = FR[d, c, k, :, at].astype(F32)
                acc = acc + PR[d, c, k, :, at].astype(F32) * jnp.concatenate([f] * nvar, axis=0)
        return acc

    def cross(c, products):
        landed((XR if products else FR).at[others, c, crossing], ar_sem.at[c])
        if not products and c == 0:
            landed(PR.at[others, pl.ds(0, npc)], pr_sem.at[1])
        if c == npc:
            landed(PR.at[others, pl.ds(npc, nc - npc)], pr_sem.at[0])

        def step(r, carry):
            at = strip(r)
            for k in range(1, o):
                YS[k, c, :, at] = summed(c, k, at, products).astype(BF16)
            return carry

        lax.fori_loop(0, cr, step, 0)
        for k in range(1, o):
            pltpu.make_async_remote_copy(
                src_ref=YS.at[k, c], dst_ref=YR.at[k, c], send_sem=send_sem.at[4], recv_sem=br_sem.at[c],
                device_id=at_outer(k), device_id_type=pl.DeviceIdType.MESH).start()

    def finish(c, products):
        landed((XR if products else FR).at[others, c, staying], zr_sem.at[c])
        landed(YR.at[crossing, c], br_sem.at[c])

        def step(r, carry):
            at = strip(r)
            acc = summed(c, 0, at, products)
            for k in range(1, o):
                acc = acc + YR[k, c, :, at].astype(F32)
            for v in range(nvar):
                out[v, :, strip(c * cr + r)] = acc[v * lm:(v + 1) * lm]
            return carry

        lax.fori_loop(0, cr, step, 0)

    def each(act, c):
        if c < npc:
            pl.when(near)(functools.partial(act, c, True))
            pl.when(far)(functools.partial(act, c, False))
        else:
            act(c, False)

    for c in range(nc):
        each(cross, c)
        for e in range(2 * c, min(nc, 2 * c + 2)):
            later(e)
    for c in range(nc):
        each(finish, c)

    peers = pl.ds(0, q - 1)
    landed(B.at[pl.ds(0, hx - rows)], send_sem.at[1])
    landed(YS.at[crossing], send_sem.at[4])

    @pl.when(near)
    def _():
        landed(PS.at[peers, pl.ds(npc, nc - npc)], send_sem.at[0])
        landed(XS.at[peers], send_sem.at[2])
        landed(FS.at[peers, pl.ds(npc, nc - npc)], send_sem.at[3])

    @pl.when(far)
    def _():
        landed(PS.at[peers], send_sem.at[0])
        landed(FS.at[peers], send_sem.at[3])


def body(nm, ng, control, kappa_table, kappa_index, tile_bounds, filter_bands, perturbation):
    _, lev, hx, hy = control.shape
    nvar, _, levels, cols = perturbation.shape
    lm = levels // nm
    rows = hx // ng
    tiles, nband, _ = filter_bands.shape
    q = inner_size(nm)
    o = nm // q
    cr = max(1, rows // 6)
    nc = rows // cr
    npc = 1
    cw = cr * hy
    dma = pltpu.SemaphoreType.DMA
    hbm = pl.BlockSpec(memory_space=pl.ANY)
    return pl.pallas_call(
        functools.partial(kernel, nm, ng, q),
        out_shape=pltpu.VMEM((nvar, lm, cols), F32),
        in_specs=[hbm] * 6,
        out_specs=pl.BlockSpec(memory_space=pltpu.VMEM),
        scratch_shapes=[
            pltpu.SMEM(kappa_table.shape, F32),
            pltpu.SMEM(tile_bounds.shape, jnp.int32),
            pltpu.VMEM((hx, lev, hy), F32),
            pltpu.VMEM((hx, lev, hy), F32),
            pltpu.VMEM((hx, lev, hy), F32),
            pltpu.VMEM((hx, lev, hy), F32),
            pltpu.VMEM((hx, lev, LANES), F32),
            pltpu.VMEM((ITERS, lev, hy), F32),
            pltpu.VMEM((hy, hy), BF16),
            pltpu.VMEM((hy, hy), BF16),
            pltpu.VMEM((hx, hy), jnp.int32),
            pltpu.VMEM((hx + 8, hy), F32),
            pltpu.VMEM((nband, tiles, levels), F32),
            pltpu.VMEM((tiles, nband, levels, LANES), F32),
            pltpu.VMEM((nband, levels, cols), F32),
            pltpu.VMEM((nvar, levels, cols), BF16),
            pltpu.VMEM((q, nc, o, nvar * lm, cw), BF16),
            pltpu.VMEM((q, nc, o, nvar * lm, cw), BF16),
            pltpu.VMEM((hx, lev, hy), BF16),
            pltpu.VMEM((ng, rows, lev, hy), BF16),
            pltpu.VMEM((levels + 16, cols), F32),
            pltpu.VMEM((q, nc, o, lm, cw), BF16),
            pltpu.VMEM((q, nc, o, lm, cw), BF16),
            pltpu.VMEM((q, npc, o, nvar * lm, cw), BF16),
            pltpu.VMEM((q, npc, o, nvar * lm, cw), BF16),
            pltpu.VMEM((o, nc, nvar * lm, cw), BF16),
            pltpu.VMEM((o, nc, nvar * lm, cw), BF16),
            dma((3,)), dma((nc,)), dma((5,)), dma((2,)), dma((nc,)), dma((nc,)), dma((nc,)), dma((nc,)),
        ],
        compiler_params=pltpu.CompilerParams(
            collective_id=0, has_side_effects=True, vmem_limit_bytes=56 * 2**20),
    )(control, kappa_table, kappa_index, tile_bounds, jnp.swapaxes(filter_bands, 0, 1), perturbation)


def solution(mesh):
    in_specs = (P("mem", "geo", None, None), P(), P(), P(), P(), P(None, "mem", None, "geo"))
    out_specs = P(None, "mem", "geo")
    run = functools.partial(body, mesh.shape["mem"], mesh.shape["geo"])
    return jax.shard_map(run, mesh=mesh, in_specs=in_specs, out_specs=out_specs, check_vma=False)
```

```python
import functools

import jax
import jax.numpy as jnp
from jax import lax
from jax.experimental import pallas as pl
from jax.experimental.pallas import tpu as pltpu
from jax.sharding import PartitionSpec as P

ITERS = 10
F32, BF16 = jnp.float32, jnp.bfloat16
LANES = 128


def inner_size(nm):
    q = 1
    while nm % (2 * q) == 0 and (2 * q) ** 2 <= 2 * nm:
        q *= 2
    return q


def kernel(nm, ng, q, ctrl, table_hbm, kidx_hbm, bounds_hbm, bands_hbm, pert_hbm, out,
           table, bounds, C, S, WE, WN, WS, FL, spread, gather, kidx, kf, bands, bandsb, coef, pert,
           PS, PR, B, G, D, FS, FR, XS, XR, YS, YR,
           loc_sem, pert_sem, send_sem, pr_sem, gr_sem, ar_sem, br_sem):
    mem = lax.axis_index("mem")
    geo = lax.axis_index("geo")
    o = nm // q
    inner = lax.rem(mem, q)
    outer = mem // q
    hx, lev, hy = S.shape
    nvar, levels, cols = pert.shape
    lm = levels // nm
    rows = hx // ng
    nband, tiles, _ = bands.shape
    parts = hy // LANES
    pad = nband // 2
    nc = YS.shape[1]
    cr = rows // nc
    cw = cr * hy
    npc = XS.shape[1]
    backward = geo < ng // 2
    near = lax.rem(geo, 2) == 1
    far = jnp.logical_not(near)

    def at_inner(d):
        return {"mem": outer * q + lax.rem(inner + d, q)}

    def at_outer(d):
        return {"mem": lax.rem(outer + d, o) * q + inner}

    barrier = pltpu.get_barrier_semaphore()
    targets = ([at_inner(d) for d in range(1, q)] + [at_outer(d) for d in range(1, o)]
               + [{"geo": lax.rem(geo + d, ng)} for d in range(1, ng)])
    for target in targets:
        pl.semaphore_signal(barrier, inc=1, device_id=target, device_id_type=pl.DeviceIdType.MESH)

    def landed(ref, sem):
        pltpu.make_async_copy(ref, ref, sem).wait()

    pert_cps = [pltpu.make_async_copy(pert_hbm.at[:, 0, :, pl.ds(c * cw, cw)], pert.at[:, :, pl.ds(c * cw, cw)], pert_sem.at[c])
                for c in range(nc)]
    for cp in pert_cps:
        cp.start()
    kidx_cp = pltpu.make_async_copy(kidx_hbm, kidx, loc_sem.at[0])
    kidx_cp.start()
    table_cp = pltpu.make_async_copy(table_hbm, table, loc_sem.at[1])
    table_cp.start()
    for l in range(lev):
        pltpu.make_async_copy(ctrl.at[0, l], C.at[:, l], loc_sem.at[2]).start()
    left = lax.broadcasted_iota(jnp.int32, (hy, hy), 0)
    right = lax.broadcasted_iota(jnp.int32, (hy, hy), 1)
    spread[...] = jnp.where(left == (right % LANES) * parts + right // LANES, 1.0, 0.0).astype(BF16)
    gather[...] = jnp.where(right == (left % LANES) * parts + left // LANES, 1.0, 0.0).astype(BF16)

    def piece(vals, i, k):
        return jnp.concatenate([v[(k * q + i) * lm:(k * q + i + 1) * lm] for v in vals], axis=0)

    def split(ref, vals, c, at):
        for k in range(o):
            slot = lax.rem(k - outer + o, o)
            for i in range(q):
                ref[i, c, slot, :, at] = piece(vals, i, k).astype(BF16)

    def strip(k):
        return pl.ds(pl.multiple_of(k * hy, LANES), hy)

    def repack(c):
        def step(r, carry):
            at = strip(c * cr + r)
            vals = [pert[v, :, at].astype(F32) for v in range(nvar)]
            split(PS, vals, c, strip(r))
            return carry

        lax.fori_loop(0, cr, step, 0)

    crossing = pl.ds(1, o - 1)
    whole = pl.ds(0, o)
    staying = pl.ds(0, 1)

    def inner_send(src, dst, c, part, send, recv):
        for d in range(1, q):
            pltpu.make_async_remote_copy(
                src_ref=src.at[lax.rem(inner + d, q), c, part], dst_ref=dst.at[d, c, part], send_sem=send, recv_sem=recv,
                device_id=at_inner(d), device_id_type=pl.DeviceIdType.MESH).start()

    def offer(c):
        repack(c)
        inner_send(PS, PR, c, whole, send_sem.at[0], pr_sem.at[0 if c >= npc else 1])

    pl.semaphore_wait(barrier, len(targets))
    for c in range(nc):
        pert_cps[c].wait()
        if c < npc:
            pl.when(far)(functools.partial(offer, c))
        else:
            offer(c)

    def turned(i, last):
        return jnp.where(backward, last - i, i)

    kidx_cp.wait()
    table_cp.wait()
    landed(C, loc_sem.at[2])
    x = C[...].reshape(hx * lev, hy)
    high = x.astype(BF16)
    low = (x - high.astype(F32)).astype(BF16)
    x = jnp.concatenate([kidx[...].astype(F32).astype(BF16), high, low], axis=0)
    x = jnp.dot(x, spread[...], preferred_element_type=F32)
    index = x[:hx]
    x = (x[hx:hx + hx * lev] + x[hx + hx * lev:]).reshape(hx, lev, hy)
    for i in range(hx):
        S[turned(i, hx - 1)] = x[i]
    field = jnp.zeros(index.shape, F32)
    for entry in range(table.shape[0]):
        field = jnp.where(index == float(entry), table[entry], field)
    kf[0:hx] = field
    kf[hx:] = jnp.zeros((kf.shape[0] - hx, hy), F32)
    east = 0.5 * (field + kf[1:hx + 1])
    lane = lax.broadcasted_iota(jnp.int32, (hx, LANES), 1)
    cut = [field[:, p * LANES:(p + 1) * LANES] for p in range(parts)]
    norths = [0.5 * (cut[p] + cut[p + 1]) for p in range(parts - 1)]
    last = 0.5 * (cut[-1] + pltpu.roll(cut[0], LANES - 1, axis=1))
    norths.append(jnp.where(lane < LANES - 1, last, 0.0))
    south = pltpu.roll(norths[-1], 1, axis=1)
    for i in range(hx):
        if i < hx - 1:
            WE[turned(i, hx - 2)] = jnp.broadcast_to(east[i:i + 1], (lev, hy))
        to = turned(i, hx - 1)
        for p in range(parts):
            WN[to, :, p * LANES:(p + 1) * LANES] = jnp.broadcast_to(norths[p][i:i + 1], (lev, LANES))
        WS[to] = jnp.broadcast_to(south[i:i + 1], (lev, LANES))

    bands_cp = pltpu.make_async_copy(bands_hbm, bands, loc_sem.at[0])
    bands_cp.start()
    bounds_cp = pltpu.make_async_copy(bounds_hbm, bounds, loc_sem.at[1])
    bounds_cp.start()

    def row_of(ref, i):
        return [ref[i, :, p * LANES:(p + 1) * LANES] for p in range(parts)]

    def sweep(it, lo, hi):
        s = row_of(S, lo)
        before = row_of(FL, it) if lo else None
        for i in range(lo, hi):
            wn = row_of(WN, i)
            ahead = s[1:] + [pltpu.roll(s[0], LANES - 1, axis=1)]
            flux = [wn[p] * (ahead[p] - s[p]) for p in range(parts)]
            behind = [WS[i] * (s[0] - pltpu.roll(s[-1], 1, axis=1))] + flux[:-1]
            new = [s[p] + (flux[p] - behind[p]) for p in range(parts)]
            if before is not None:
                new = [new[p] - before[p] for p in range(parts)]
            if i < hx - 1:
                after = row_of(S, i + 1)
                we = row_of(WE, i)
                before = [we[p] * (after[p] - s[p]) for p in range(parts)]
                new = [new[p] + before[p] for p in range(parts)]
                s = after
            for p in range(parts):
                S[i, :, p * LANES:(p + 1) * LANES] = new[p]
        if hi < hx:
            for p in range(parts):
                FL[it, :, p * LANES:(p + 1) * LANES] = before[p]

    half = ng // 2
    span = half * rows
    for b in range(2):
        for it in range(ITERS):
            lo, hi = (0, min(hx, span + ITERS - 1 - it)) if b == 0 else (min(hx, span + ITERS - 1 - it), hx)
            if hi > lo:
                sweep(it, lo, hi)
        if (span * lev) % 8 == 0:
            x = S[b * span:(b + 1) * span].reshape(span * lev, hy).astype(BF16)
            x = jnp.dot(x, gather[...], preferred_element_type=F32).reshape(span, lev, hy).astype(BF16)
        else:
            x = [jnp.dot(S[b * span + r].astype(BF16), gather[...], preferred_element_type=F32).astype(BF16)
                 for r in range(span)]
        for r in range(span):
            B[turned(b * span + r, hx - 1)] = x[r]
        for j in range(half):
            band = j + jnp.where(backward, half, 0) if b == 0 else j + jnp.where(backward, 0, half)
            cps = [pltpu.make_async_remote_copy(
                src_ref=B.at[pl.ds(band * rows + c * cr, cr)], dst_ref=G.at[geo, pl.ds(c * cr, cr)],
                send_sem=send_sem.at[1], recv_sem=gr_sem.at[c],
                device_id={"geo": band}, device_id_type=pl.DeviceIdType.MESH) for c in range(nc)]
            if b == 0:
                for cp in cps:
                    cp.start()
            else:
                @pl.when(band != geo)
                def _(cps=cps):
                    for cp in cps:
                        cp.start()

    for c in range(nc):
        pltpu.make_async_copy(B.at[pl.ds(geo * rows + c * cr, cr)], G.at[geo, pl.ds(c * cr, cr)], gr_sem.at[c]).start()

    bands_cp.wait()
    bounds_cp.wait()
    eye = (lax.broadcasted_iota(jnp.int32, (levels, levels), 0)
           == lax.broadcasted_iota(jnp.int32, (levels, levels), 1))
    for t in range(tiles):
        for k in range(nband):
            row = jnp.broadcast_to(bands[k, t:t + 1, :], (levels, levels))
            column = jnp.sum(jnp.where(eye, row, 0.0), axis=1, keepdims=True)
            bandsb[t, k] = jnp.broadcast_to(column, (levels, LANES))

    def coefficients(k, carry):
        at = pl.ds(pl.multiple_of(k * LANES, LANES), LANES)
        column = geo * cols + k * LANES + lax.broadcasted_iota(jnp.int32, (levels, LANES), 1)
        past = [column >= bounds[t] for t in range(1, tiles)]
        for k in range(nband):
            value = bandsb[0, k]
            for t in range(1, tiles):
                value = jnp.where(past[t - 1], bandsb[t, k], value)
            coef[k, :, at] = value
        return carry

    lax.fori_loop(0, cols // LANES, coefficients, 0)
    base = 8
    D[0:base, :] = jnp.zeros((base, cols), F32)
    D[base + levels:, :] = jnp.zeros((D.shape[0] - base - levels, cols), F32)

    def filtered(k):
        at = strip(k)
        value = D[base:base + levels, at]
        for n in range(nband):
            value = value + coef[n, :, at] * D[base + n - pad:base + n - pad + levels, at]
        return value.astype(BF16).astype(F32), at

    def vertical(c, products):
        def step(r, carry):
            k = c * cr + r
            for g in range(ng):
                D[base + g * lev:base + (g + 1) * lev, strip(k)] = G[g, k].astype(F32)
            value, at = filtered(k)
            if products:
                vals = [pert[v, :, at].astype(F32) * value for v in range(nvar)]
                split(XS, vals, c, strip(r))
            else:
                split(FS, [value], c, strip(r))
            return carry

        lax.fori_loop(0, cr, step, 0)

    def hand(c, products, part, send, recv):
        if products:
            inner_send(XS, XR, c, part, send, recv.at[c])
        else:
            inner_send(FS, FR, c, part, send, recv.at[c])

    def vertical_send(c, products, send):
        vertical(c, products)
        hand(c, products, crossing, send, ar_sem)

    for c in range(nc):
        landed(G.at[:, pl.ds(c * cr, cr)], gr_sem.at[c])
        if c < npc:
            pl.when(near)(functools.partial(vertical_send, c, True, send_sem.at[2]))
            pl.when(far)(functools.partial(vertical_send, c, False, send_sem.at[3]))
        else:
            vertical_send(c, False, send_sem.at[3])

    def later(c):
        if c < npc:
            pl.when(near)(functools.partial(hand, c, True, staying, send_sem.at[2], pert_sem))
            pl.when(far)(functools.partial(hand, c, False, staying, send_sem.at[3], pert_sem))
        else:
            hand(c, False, staying, send_sem.at[3], pert_sem)

    others = pl.ds(1, q - 1)

    def summed(c, k, at, products):
        if products:
            acc = XS[inner, c, k, :, at].astype(F32)
            for d in range(1, q):
                acc = acc + XR[d, c, k, :, at].astype(F32)
        else:
            f = FS[inner, c, k, :, at].astype(F32)
            acc = PS[inner, c, k, :, at].astype(F32) * jnp.concatenate([f] * nvar, axis=0)
            for d in range(1, q):
                f = FR[d, c, k, :, at].astype(F32)
                acc = acc + PR[d, c, k, :, at].astype(F32) * jnp.concatenate([f] * nvar, axis=0)
        return acc

    def cross(c, products):
        landed((XR if products else FR).at[others, c, crossing], ar_sem.at[c])
        if not products and c == 0:
            landed(PR.at[others, pl.ds(0, npc)], pr_sem.at[1])
        if c == npc:
            landed(PR.at[others, pl.ds(npc, nc - npc)], pr_sem.at[0])

        def step(r, carry):
            at = strip(r)
            for k in range(1, o):
                YS[k, c, :, at] = summed(c, k, at, products).astype(BF16)
            return carry

        lax.fori_loop(0, cr, step, 0)
        for k in range(1, o):
            pltpu.make_async_remote_copy(
                src_ref=YS.at[k, c], dst_ref=YR.at[k, c], send_sem=send_sem.at[4], recv_sem=br_sem.at[c],
                device_id=at_outer(k), device_id_type=pl.DeviceIdType.MESH).start()

    def finish(c, products):
        landed((XR if products else FR).at[others, c, staying], pert_sem.at[c])
        landed(YR.at[crossing, c], br_sem.at[c])

        def step(r, carry):
            at = strip(r)
            acc = summed(c, 0, at, products)
            for k in range(1, o):
                acc = acc + YR[k, c, :, at].astype(F32)
            for v in range(nvar):
                out[v, :, strip(c * cr + r)] = acc[v * lm:(v + 1) * lm]
            return carry

        lax.fori_loop(0, cr, step, 0)

    def each(act, c):
        if c < npc:
            pl.when(near)(functools.partial(act, c, True))
            pl.when(far)(functools.partial(act, c, False))
        else:
            act(c, False)

    for c in range(nc):
        each(cross, c)
        for e in range(2 * c, min(nc, 2 * c + 2)):
            later(e)
    for c in range(nc):
        each(finish, c)

    peers = pl.ds(0, q - 1)
    landed(B.at[pl.ds(0, hx - rows)], send_sem.at[1])
    landed(YS.at[crossing], send_sem.at[4])

    @pl.when(near)
    def _():
        landed(PS.at[peers, pl.ds(npc, nc - npc)], send_sem.at[0])
        landed(XS.at[peers], send_sem.at[2])
        landed(FS.at[peers, pl.ds(npc, nc - npc)], send_sem.at[3])

    @pl.when(far)
    def _():
        landed(PS.at[peers], send_sem.at[0])
        landed(FS.at[peers], send_sem.at[3])


def body(nm, ng, control, kappa_table, kappa_index, tile_bounds, filter_bands, perturbation):
    _, lev, hx, hy = control.shape
    nvar, _, levels, cols = perturbation.shape
    lm = levels // nm
    rows = hx // ng
    tiles, nband, _ = filter_bands.shape
    q = inner_size(nm)
    o = nm // q
    cr = max(1, rows // 6)
    nc = rows // cr
    npc = 1
    cw = cr * hy
    dma = pltpu.SemaphoreType.DMA
    hbm = pl.BlockSpec(memory_space=pl.ANY)
    return pl.pallas_call(
        functools.partial(kernel, nm, ng, q),
        out_shape=pltpu.VMEM((nvar, lm, cols), F32),
        in_specs=[hbm] * 6,
        out_specs=pl.BlockSpec(memory_space=pltpu.VMEM),
        scratch_shapes=[
            pltpu.SMEM(kappa_table.shape, F32),
            pltpu.SMEM(tile_bounds.shape, jnp.int32),
            pltpu.VMEM((hx, lev, hy), F32),
            pltpu.VMEM((hx, lev, hy), F32),
            pltpu.VMEM((hx, lev, hy), F32),
            pltpu.VMEM((hx, lev, hy), F32),
            pltpu.VMEM((hx, lev, LANES), F32),
            pltpu.VMEM((ITERS, lev, hy), F32),
            pltpu.VMEM((hy, hy), BF16),
            pltpu.VMEM((hy, hy), BF16),
            pltpu.VMEM((hx, hy), jnp.int32),
            pltpu.VMEM((hx + 8, hy), F32),
            pltpu.VMEM((nband, tiles, levels), F32),
            pltpu.VMEM((tiles, nband, levels, LANES), F32),
            pltpu.VMEM((nband, levels, cols), F32),
            pltpu.VMEM((nvar, levels, cols), BF16),
            pltpu.VMEM((q, nc, o, nvar * lm, cw), BF16),
            pltpu.VMEM((q, nc, o, nvar * lm, cw), BF16),
            pltpu.VMEM((hx, lev, hy), BF16),
            pltpu.VMEM((ng, rows, lev, hy), BF16),
            pltpu.VMEM((levels + 16, cols), F32),
            pltpu.VMEM((q, nc, o, lm, cw), BF16),
            pltpu.VMEM((q, nc, o, lm, cw), BF16),
            pltpu.VMEM((q, npc, o, nvar * lm, cw), BF16),
            pltpu.VMEM((q, npc, o, nvar * lm, cw), BF16),
            pltpu.VMEM((o, nc, nvar * lm, cw), BF16),
            pltpu.VMEM((o, nc, nvar * lm, cw), BF16),
            dma((3,)), dma((nc,)), dma((5,)), dma((2,)), dma((nc,)), dma((nc,)), dma((nc,)),
        ],
        compiler_params=pltpu.CompilerParams(
            collective_id=0, has_side_effects=True, vmem_limit_bytes=56 * 2**20),
    )(control, kappa_table, kappa_index, tile_bounds, jnp.swapaxes(filter_bands, 0, 1), perturbation)


def solution(mesh):
    in_specs = (P("mem", "geo", None, None), P(), P(), P(), P(), P(None, "mem", None, "geo"))
    out_specs = P(None, "mem", "geo")
    run = functools.partial(body, mesh.shape["mem"], mesh.shape["geo"])
    return jax.shard_map(run, mesh=mesh, in_specs=in_specs, out_specs=out_specs, check_vma=False)
```
